32 devices in a mesh: row: 4 (over x, core), col: 8 (over z, y).
Axes of the slice: x: 2, y: 2, z: 4, core: 2. Of those that a mesh axis runs over, the one named last changes fastest.
Arguments:
- x_vals: bfloat16 [256, 32, 4096], P(('row', 'col')), may hold values from -6 to 6
- occupancy: int32 [256, 32], P(('row', 'col')), may hold values from 0 to 1, as said below
- perm: int32 [256], replicated, may hold values from 0 to 255, as said below
Outputs:
- sign_iterate_next: bfloat16 [16384, 16384], P('row', 'col')
The draws below stay inside these ranges and needn't reach their ends.
Inputs may be any that keep to these rules, and one draw needn't show every extreme that they name: occupancy[i, s] = 1 marks block (i, (i - 16 + s) mod 256) as present; the diagonal slot s = 16 is always 1, and some row has all 32 slots 1. perm is a permutation with perm[j] = a(j mod (8)) * 32 + b(j div (8)) for permutations a and b; so the 32 band columns of any row fall exactly 4 times into each aligned run of 32 new indices, and each aligned run of 64 initial indices has exactly 16 members in each aligned run of 64 new indices.
All inputs are finite; a program needn't handle non-finite values.
Results may differ from the reference program's by a relative error of at most 0.0017.
Values may be sent and summed in bfloat16 or wider, within the bound.
A program may use at most 128 MiB of HBM per device.

```python
import jax
import jax.numpy as jnp
from jax import lax

BLOCK_EDGE = 64
NB = 256
W = 32
CP = 32


def draw_occupancy(key, part):
    key_keep = jax.random.fold_in(key, 11)
    key_full = jax.random.fold_in(key, 12)
    key_pick = jax.random.fold_in(key, 13)
    kept_slots = jax.random.randint(key_keep, (NB, W), 0, 5) < 3
    full_rows = jax.random.randint(key_full, (NB,), 0, 8) == 0
    forced = jnp.arange(NB) == jax.random.randint(key_pick, (), 0, NB)
    diagonal = (jnp.arange(W) == W // 2)[None, :]
    present_mask = kept_slots | diagonal | (full_rows | forced)[:, None]
    return present_mask.astype(jnp.int32)


def draw_perm(key, part):
    residues = NB // CP
    column_map = jax.random.permutation(jax.random.fold_in(key, 21), residues)
    within_map = jax.random.permutation(jax.random.fold_in(key, 22), CP)
    index_all = jnp.arange(NB)
    return (column_map[index_all % residues] * CP + within_map[index_all // residues]).astype(jnp.int32)


def block_scale(own_key, shape, cuts, smallest, top_value):
    def one(dim, parts):
        heights = jax.random.uniform(jax.random.fold_in(jax.random.fold_in(own_key, 6), dim), (parts,), jnp.float32, smallest / len(cuts), top_value / len(cuts))
        return jnp.repeat(jnp.exp(heights), shape[dim] // parts).reshape((-1,) + (1,) * (len(shape) - dim - 1))

    factor_of = one(*cuts[0])
    for cut in cuts[1:]:
        factor_of = factor_of * one(*cut)
    return factor_of


def scatter_about(rng, dims, width, limit, shards=(), kind=jnp.bfloat16):
    array = jax.random.normal(rng, dims, jnp.float32) * width
    if len(shards) > 0:
        array = block_scale(rng, dims, shards, -0.22, 0.18) * array
    return jnp.clip(array, min=-limit, max=limit).astype(kind)


def setup_inputs(seed: int = 0) -> dict:
    seeds = jax.random.split(jax.random.key(seed), 4)
    return {
        "x_vals": scatter_about(seeds[0], (NB, W, BLOCK_EDGE * BLOCK_EDGE), 1.0, 6.0, ((0, 32),)),
        "occupancy": draw_occupancy(jax.random.fold_in(seeds[3], 71), 0),
        "perm": draw_perm(jax.random.fold_in(seeds[3], 71), 0),
    }


def filtered_rows(left_vals, right_vals, block_cols):
    band_extent = block_cols.shape[1]
    slot_ids = jnp.arange(band_extent, dtype=jnp.int32)

    def one_row(inputs):
        row_vals, row_cols = inputs
        present_mask = row_cols >= 0
        source = jnp.where(present_mask, row_cols, 0).astype(jnp.int32)
        found_cols = block_cols[source]
        matched = (found_cols[:, None, :] == row_cols[None, :, None]) & present_mask[:, None, None] & present_mask[None, :, None]
        located = jnp.any(matched, axis=2)
        which_slot = jnp.sum(matched.astype(jnp.int32) * slot_ids[None, None, :], axis=2).astype(jnp.int32)
        chosen = right_vals[source[:, None], which_slot]
        chosen = jnp.where(located[:, :, None], chosen, jnp.zeros_like(chosen))
        left_factor_blocks = row_vals.reshape(band_extent, BLOCK_EDGE, BLOCK_EDGE).astype(jnp.float32)
        right_factor_blocks = chosen.reshape(band_extent, band_extent, BLOCK_EDGE, BLOCK_EDGE).astype(jnp.float32)
        return jnp.einsum("exp,egpk->gxk", left_factor_blocks, right_factor_blocks).reshape(band_extent, BLOCK_EDGE * BLOCK_EDGE)

    return lax.map(one_row, (left_vals, block_cols))


def reference(x_vals, occupancy, perm):
    index_all = jnp.arange(NB, dtype=jnp.int32)
    inverse = jnp.zeros((NB,), jnp.int32).at[perm].set(index_all)
    orig_cols = (index_all[:, None] - W // 2 + jnp.arange(W, dtype=jnp.int32)[None, :]) % NB
    present_mask = occupancy == 1
    new_cols = jnp.where(present_mask, perm[orig_cols], -1).astype(jnp.int32)
    kept_vals = jnp.where(present_mask[:, :, None], x_vals, jnp.zeros_like(x_vals))
    relaid = kept_vals[inverse]
    relaid_cols = new_cols[inverse]
    square = filtered_rows(relaid, relaid, relaid_cols).astype(jnp.bfloat16)
    cube_vals = filtered_rows(relaid, square, relaid_cols)
    stepped_matrix = (1.5 * relaid.astype(jnp.float32) - (0.5 / (BLOCK_EDGE * W)) * cube_vals).astype(jnp.bfloat16)
    alive_slot = relaid_cols >= 0
    stepped_matrix = jnp.where(alive_slot[:, :, None], stepped_matrix, jnp.zeros_like(stepped_matrix))
    target = jnp.where(alive_slot, relaid_cols, 0).astype(jnp.int32)
    blocks = jnp.zeros((NB, NB, BLOCK_EDGE * BLOCK_EDGE), jnp.bfloat16).at[index_all[:, None], target].add(stepped_matrix)
    return blocks.reshape(NB, NB, BLOCK_EDGE, BLOCK_EDGE).transpose(0, 2, 1, 3).reshape(NB * BLOCK_EDGE, NB * BLOCK_EDGE)
```

```python
import functools

import jax
import jax.numpy as jnp
from jax import lax
from jax.experimental import pallas as pl
from jax.experimental.pallas import tpu as pltpu
from jax.sharding import PartitionSpec as P

BLOCK_EDGE = 64
MESH = pl.DeviceIdType.MESH
ANY = pl.BlockSpec(memory_space=pl.ANY)


def multiply_kernel(order_ref, left_ref, far0, far1, far2, far3, out_ref):
    width = out_ref.shape[-1]
    left = left_ref[...].reshape(-1, width)
    right = jnp.concatenate([r[...].reshape(-1, width) for r in (far0, far1, far2, far3)], axis=0)
    update = jnp.dot(left, right, preferred_element_type=jnp.float32).reshape(out_ref.shape)

    @pl.when(pl.program_id(1) == 0)
    def _():
        out_ref[...] = update

    @pl.when(pl.program_id(1) != 0)
    def _():
        out_ref[...] += update


def banded_product(left, far, order, residue_major, slots):
    panels, halves, count, edge, width = left.shape
    chunk = slots // 2
    chunks = count // chunk

    def far_spec(position):
        def chunk_of(g):
            return lax.rem(2 * g + chunks - 1 + lax.rem(position + 1 + 2 * g, 4), chunks)

        if residue_major:
            return pl.BlockSpec(
                (1, chunk, edge, width), lambda g, p, order: (order[p], chunk_of(g), 0, 0)
            )
        return pl.BlockSpec(
            (chunk, 1, edge, width), lambda g, p, order: (chunk_of(g), order[p], 0, 0)
        )

    return pl.pallas_call(
        multiply_kernel,
        out_shape=jax.ShapeDtypeStruct((halves, count, edge, width), jnp.float32),
        grid_spec=pltpu.PrefetchScalarGridSpec(
            num_scalar_prefetch=1,
            grid=(count // slots, panels),
            in_specs=[
                pl.BlockSpec(
                    (1, halves, slots, edge, width), lambda g, p, order: (p, 0, g, 0, 0)
                )
            ]
            + [far_spec(position) for position in range(4)],
            out_specs=pl.BlockSpec((halves, slots, edge, width), lambda g, p, order: (0, g, 0, 0)),
        ),
        compiler_params=pltpu.CompilerParams(dimension_semantics=("arbitrary", "arbitrary")),
    )(order, left, far, far, far, far)


def spread_kernel(source_ref, target_ref, rows_ref, out_ref):
    slots = rows_ref.shape[-1] // BLOCK_EDGE
    q, n = pl.program_id(0), pl.program_id(1)
    row = q * pl.num_programs(1) + source_ref[n]
    out_ref[...] = jnp.zeros_like(out_ref)
    for v in range(slots):
        block = rows_ref[0, 0, :, v * BLOCK_EDGE : (v + 1) * BLOCK_EDGE].astype(jnp.float32)
        target = target_ref[row * slots + v]
        odd = lax.rem(target, 2)
        pair = jnp.concatenate(
            [block * (1 - odd).astype(jnp.float32), block * odd.astype(jnp.float32)], axis=1
        ).astype(out_ref.dtype)
        at = pl.multiple_of((target // 2) * (2 * BLOCK_EDGE), 2 * BLOCK_EDGE)
        out_ref[:, pl.ds(at, 2 * BLOCK_EDGE)] += pair


def spread(rows, source, target, panel_cols):
    halves, count, edge, width = rows.shape
    return pl.pallas_call(
        spread_kernel,
        out_shape=jax.ShapeDtypeStruct((halves * count * edge, panel_cols * edge), rows.dtype),
        grid_spec=pltpu.PrefetchScalarGridSpec(
            num_scalar_prefetch=2,
            grid=(halves, count),
            in_specs=[
                pl.BlockSpec((1, 1, edge, width), lambda q, n, source, target: (q, source[n], 0, 0))
            ],
            out_specs=pl.BlockSpec(
                (edge, panel_cols * edge), lambda q, n, source, target: (q * count + n, 0)
            ),
        ),
        compiler_params=pltpu.CompilerParams(dimension_semantics=("arbitrary", "arbitrary")),
    )(source, target, rows)


def band_index(m, row_residue, col_residue, slots):
    first = m - slots // 2 + (col_residue < row_residue).astype(jnp.int32)
    v = jnp.arange(slots, dtype=jnp.int32)
    first = first[..., None]
    return first + (v - first) % slots


def widen(values, index, slots):
    high = (index % (2 * slots)) >= slots
    high = jnp.repeat(high, BLOCK_EDGE, axis=-1)[..., None, :]
    zero = jnp.zeros((), values.dtype)
    return jnp.concatenate(
        [jnp.where(high, zero, values), jnp.where(high, values, zero)], axis=-1
    )


def panel_shards(x_vals, occupancy, perm):
    row_devices = lax.axis_size("row")
    panels = lax.axis_size("col")
    own_row = lax.axis_index("row")
    own_col = lax.axis_index("col")
    local_rows, band_extent, block_area = x_vals.shape
    block_count = perm.shape[0]
    panel_cols = block_count // panels
    halves = panels // row_devices
    slots = band_extent // panels
    lanes = slots * BLOCK_EDGE

    panel_of_residue = perm[:panels] // panel_cols
    residue_ids = jnp.arange(panels, dtype=jnp.int32)
    order = jnp.sum(
        jnp.where(panel_of_residue[None, :] == residue_ids[:, None], residue_ids[None, :], 0), axis=1
    ).astype(jnp.int32)
    inside = perm[::panels] % panel_cols
    m_ids = jnp.arange(panel_cols, dtype=jnp.int32)
    source = jnp.sum(
        jnp.where(inside[None, :] == m_ids[:, None], m_ids[None, :], 0), axis=1
    ).astype(jnp.int32)
    own_residue = order[own_col]
    row_residues = lax.dynamic_slice_in_dim(order, own_row * halves, halves)

    first_row = (own_row * panels + own_col) * local_rows
    row_ids = first_row + jnp.arange(local_rows, dtype=jnp.int32)
    cols = (
        row_ids[:, None] - band_extent // 2 + jnp.arange(band_extent, dtype=jnp.int32)[None, :]
    ) % block_count
    placed = (
        (occupancy[:, :, None, None] == 1)
        & ((cols % panels)[:, :, None, None] == order[None, None, :, None])
        & (
            ((cols // panels) % slots)[:, :, None, None]
            == jnp.arange(slots, dtype=jnp.int32)[None, None, None, :]
        )
    ).astype(jnp.bfloat16)
    kept = jnp.sum(placed.astype(jnp.float32), axis=1).astype(jnp.bfloat16)
    every_kept = lax.all_gather(
        kept.reshape(local_rows, panels * slots), ("row", "col"), axis=0, tiled=True
    ).reshape(panel_cols, panels, panels, slots)
    values = jnp.einsum(
        "kspt,ksf->pktf", placed, x_vals, preferred_element_type=jnp.float32
    ).astype(jnp.bfloat16)
    values = (
        values.reshape(panels, local_rows, slots, BLOCK_EDGE, BLOCK_EDGE)
        .transpose(0, 1, 3, 2, 4)
        .reshape(panels, local_rows, BLOCK_EDGE, lanes)
    )
    first = lax.all_to_all(values, "col", split_axis=0, concat_axis=0, tiled=True)
    first = first.reshape(panels * local_rows, BLOCK_EDGE, lanes)
    far = lax.all_gather(first, "row", axis=0, tiled=True).reshape(
        panel_cols, panels, BLOCK_EDGE, lanes
    )
    tile = jnp.stack(
        [
            lax.dynamic_index_in_dim(far, row_residues[q], axis=1, keepdims=False)
            for q in range(halves)
        ]
    )
    own_kept = lax.dynamic_index_in_dim(every_kept, own_col, axis=2, keepdims=False)
    wanted = jnp.stack(
        [
            lax.dynamic_index_in_dim(own_kept, row_residues[q], axis=1, keepdims=False)
            for q in range(halves)
        ]
    )
    wanted = wanted > 0
    left = lax.all_gather(tile[None], "col", axis=0, tiled=True)

    far_index = band_index(m_ids[:, None], residue_ids[None, :], own_residue, slots)
    far_wide = widen(far, far_index, slots)
    left_index = band_index(
        m_ids[None, None, :], row_residues[None, :, None], order[:, None, None], slots
    )
    left_wide = widen(left, left_index, slots)
    tile_index = band_index(m_ids[None, :], row_residues[:, None], own_residue, slots)
    tile_high = (tile_index % (2 * slots)) >= slots

    def spread_mask(mask):
        return jnp.repeat(mask, BLOCK_EDGE, axis=-1)[:, :, None, :]

    def narrow(wide):
        chosen = jnp.where(spread_mask(tile_high), wide[..., lanes:], wide[..., :lanes])
        return jnp.where(spread_mask(wanted), chosen, 0.0)

    square = narrow(banded_product(left_wide, far_wide, order, False, slots)).astype(jnp.bfloat16)
    far_square = lax.all_gather(square, "row", axis=0, tiled=True)
    square_index = band_index(m_ids[None, :], order[:, None], own_residue, slots)
    square_wide = widen(far_square, square_index, slots)
    cube = narrow(banded_product(left_wide, square_wide, residue_ids, True, slots))
    stepped = (
        1.5 * tile.astype(jnp.float32) - 0.5 / (BLOCK_EDGE * band_extent) * cube
    ).astype(jnp.bfloat16)
    hit = (tile_index % panel_cols)[..., None] == m_ids
    target = jnp.sum(jnp.where(hit, inside, 0), axis=-1).astype(jnp.int32).reshape(-1)
    return spread(stepped, source, target, panel_cols)


class Place:
    def __init__(self, panels):
        self.depth = panels // 2
        self.quarter = panels // 4
        row, col = lax.axis_index("row"), lax.axis_index("col")
        self.half, self.core = row // 2, row % 2
        self.level, self.lane = col // 2, col % 2
        self.step = jnp.where(self.half == 0, self.level, self.depth - 1 - self.level)
        self.ring = self.half * self.depth + self.step

    def device(self, half, core, level, lane):
        return (2 * half + core, 2 * level + lane)

    def at_ring(self, ring):
        half = ring // self.depth
        step = ring % self.depth
        level = jnp.where(half == 0, step, self.depth - 1 - step)
        return self.device(half, self.core, level, self.lane)

    def neighbour(self, by):
        return self.at_ring((self.ring + by + 2 * self.depth) % (2 * self.depth))

    def group_target(self):
        step = self.core * self.quarter + self.level // 2
        level = jnp.where(self.half == 0, step, self.depth - 1 - step)
        return self.device(self.half, 1 - self.level % 2, level, self.lane)

    def group_source(self):
        level = 2 * (self.step % self.quarter) + 1 - self.core
        return self.device(self.half, self.step // self.quarter, level, self.lane)


def greet(devices):
    barrier = pltpu.get_barrier_semaphore()
    for device in devices:
        pl.semaphore_signal(barrier, inc=1, device_id=device, device_id_type=MESH)
    pl.semaphore_wait(barrier, len(devices))


def remote(source, target, send, recv, device):
    return pltpu.make_async_remote_copy(
        src_ref=source,
        dst_ref=target,
        send_sem=send,
        recv_sem=recv,
        device_id=device,
        device_id_type=MESH,
    )


def gather_kernel(panels, rows, marks, all_rows, all_marks, *sems):
    place = Place(panels)
    count = rows.shape[0]
    over_level, over_lane, over_core, relayed = [sems[2 * n : 2 * n + 2] for n in range(4)]
    target, source = place.group_target(), place.group_source()
    lane_peer = place.device(place.half, place.core, place.level, 1 - place.lane)
    core_peer = place.device(place.half, 1 - place.core, place.level, place.lane)
    target_slot = 2 * (place.level % 2) + place.lane
    own_slot = 2 * (1 - place.core) + place.lane
    peer_slot = 2 * (1 - place.core) + 1 - place.lane
    greet((source, lane_peer, core_peer))

    def piece(slot, n):
        return all_marks.at[slot] if n == 0 else all_rows.at[slot, n - 1]

    def copies(sem, device, slot, first=False):
        out = []
        for n in range(count + 1):
            origin = (marks if n == 0 else rows.at[n - 1]) if first else piece(slot, n)
            out.append(remote(origin, piece(slot, n), sem[0].at[n], sem[1].at[n], device))
        return out

    moves = copies(over_level, target, target_slot, True)
    lanes = copies(over_lane, lane_peer, own_slot)
    cores = copies(over_core, core_peer, own_slot)
    relays = copies(relayed, core_peer, peer_slot)
    for move in moves:
        move.start()
    for move, lane, core in zip(moves, lanes, cores):
        move.wait_recv()
        lane.start()
        core.start()
    for lane, relay in zip(lanes, relays):
        lane.wait_recv()
        relay.start()
    for core, relay in zip(cores, relays):
        core.wait_recv()
        relay.wait_recv()
    for group in (moves, lanes, cores, relays):
        for copy in group:
            copy.wait_send()


def gather_groups(rows, marks, panels):
    count = rows.shape[0]
    sems = [pltpu.SemaphoreType.DMA((count + 1,)) for _ in range(8)]
    return pl.pallas_call(
        functools.partial(gather_kernel, panels),
        out_shape=(
            jax.ShapeDtypeStruct((4,) + rows.shape, rows.dtype),
            jax.ShapeDtypeStruct((4,) + marks.shape, marks.dtype),
        ),
        in_specs=[ANY, ANY],
        out_specs=(ANY, ANY),
        scratch_shapes=sems,
        compiler_params=pltpu.CompilerParams(collective_id=0, has_side_effects=True),
        name="gather_groups",
    )(rows, marks)


def lay_kernel(rows_ref, marks_ref, pick_ref, left_ref, right_ref, kept_ref):
    count, edge, lanes = rows_ref.shape[1:]
    octet = count * edge
    rest = left_ref.shape[-1] - lanes
    for t in range(count):
        row = rows_ref[0, t]
        parts = [row]
        if t:
            parts = [jnp.zeros((edge, t * edge), row.dtype)] + parts
        if rest - t * edge:
            parts = parts + [jnp.zeros((edge, rest - t * edge), row.dtype)]
        left_ref[0, t * edge : (t + 1) * edge, :] = jnp.concatenate(parts, axis=1)
    pick = pick_ref[...]
    width = pick.shape[1]
    for o in range(left_ref.shape[-1] // octet):
        at, to = slice(o * octet, (o + 1) * octet), slice(o * width, (o + 1) * width)
        right_ref[0, :, to] = jnp.dot(
            left_ref[0, :, at], pick, preferred_element_type=jnp.float32
        ).astype(right_ref.dtype)
        kept_ref[0, :, to] = jnp.dot(
            marks_ref[0, :, at], pick, preferred_element_type=jnp.float32
        )


def lay_out(rows, marks, pick):
    groups, count, edge, lanes = rows.shape
    octet, width = pick.shape
    wide = marks.shape[-1]
    narrow = wide // octet * width
    return pl.pallas_call(
        lay_kernel,
        out_shape=(
            jax.ShapeDtypeStruct((groups, octet, wide), rows.dtype),
            jax.ShapeDtypeStruct((groups + 4, octet, narrow), rows.dtype),
            jax.ShapeDtypeStruct((groups, count, narrow), jnp.float32),
        ),
        grid=(groups,),
        in_specs=[
            pl.BlockSpec((1, count, edge, lanes), lambda g: (g, 0, 0, 0)),
            pl.BlockSpec((1, count, wide), lambda g: (g, 0, 0)),
            pl.BlockSpec((octet, width), lambda g: (0, 0)),
        ],
        out_specs=(
            pl.BlockSpec((1, octet, wide), lambda g: (g, 0, 0)),
            pl.BlockSpec((1, octet, narrow), lambda g: (g + 2, 0, 0)),
            pl.BlockSpec((1, count, narrow), lambda g: (g, 0, 0)),
        ),
        compiler_params=pltpu.CompilerParams(dimension_semantics=("arbitrary",)),
        name="lay_out",
    )(rows, marks, pick)


def halo_kernel(panels, tiles_in, tiles, send, recv):
    del tiles_in
    place = Place(panels)
    after, before = place.neighbour(1), place.neighbour(-1)
    groups = tiles.shape[0] - 4
    wide = tiles.shape[-1]
    step = wide // 5
    greet((after, before))
    moves = (
        (groups, 0, slice(2 * step, wide), after),
        (groups + 1, 1, slice(step, wide), after),
        (2, groups + 2, slice(0, 4 * step), before),
        (3, groups + 3, slice(0, 3 * step), before),
    )
    copies = [
        remote(
            tiles.at[origin, :, lanes], tiles.at[to, :, lanes], send.at[n], recv.at[n], device
        )
        for n, (origin, to, lanes, device) in enumerate(moves)
    ]
    for copy in copies:
        copy.start()
    for copy in copies:
        copy.wait()


def exchange_halo(tiles, panels, collective_id):
    return pl.pallas_call(
        functools.partial(halo_kernel, panels),
        out_shape=jax.ShapeDtypeStruct(tiles.shape, tiles.dtype),
        in_specs=[ANY],
        out_specs=ANY,
        scratch_shapes=[pltpu.SemaphoreType.DMA((4,)), pltpu.SemaphoreType.DMA((4,))],
        input_output_aliases={0: 0},
        compiler_params=pltpu.CompilerParams(
            collective_id=collective_id, has_side_effects=True
        ),
        name="exchange_halo",
    )(tiles)


def multiply(left_ref, tiles_ref, total):
    t = pl.program_id(0)
    depth, wide = tiles_ref.shape[1:]
    step = wide // 5
    for n, (at, to) in enumerate(((0, 0), (-1, 0), (-2, 0), (1, 1), (2, 2))):
        reach = wide - abs(at) * step
        first = 0 if at >= 0 else wide - reach
        tile = tiles_ref[t + 2 + at, :, first : first + reach]
        update = jnp.dot(
            left_ref[0, :, (2 + at) * depth : (3 + at) * depth],
            tile,
            preferred_element_type=jnp.float32,
        )
        if n == 0:
            total[...] = update
        else:
            total[:, to * step : to * step + reach] += update


def square_kernel(left_ref, tiles_ref, kept_ref, out_ref, total):
    multiply(left_ref, tiles_ref, total)
    count = kept_ref.shape[1]
    edge = total.shape[0] // count
    for r in range(count):
        at = slice(r * edge, (r + 1) * edge)
        out_ref[0, at, :] = (total[at, :] * kept_ref[0, r : r + 1, :]).astype(out_ref.dtype)


def square_tiles(left, tiles, kept):
    groups, octet, wide = left.shape
    narrow = tiles.shape[-1]
    return pl.pallas_call(
        square_kernel,
        out_shape=jax.ShapeDtypeStruct(tiles.shape, tiles.dtype),
        grid=(groups,),
        in_specs=[
            pl.BlockSpec((1, octet, wide), lambda g: (g, 0, 0)),
            pl.BlockSpec(tiles.shape, lambda g: (0, 0, 0)),
            pl.BlockSpec((1,) + kept.shape[1:], lambda g: (g, 0, 0)),
        ],
        out_specs=pl.BlockSpec((1, octet, narrow), lambda g: (g + 2, 0, 0)),
        scratch_shapes=[pltpu.VMEM((octet, narrow), jnp.float32)],
        compiler_params=pltpu.CompilerParams(dimension_semantics=("arbitrary",)),
        name="square_tiles",
    )(left, tiles, kept)


def step_kernel(
    scale, residues, order, left_ref, tiles_ref, own_ref, kept_ref, out_ref, total
):
    multiply(left_ref, tiles_ref, total)
    count = kept_ref.shape[1]
    edge = total.shape[0] // count
    for r in range(count):
        at = slice(r * edge, (r + 1) * edge)
        total[at, :] = 1.5 * own_ref[0, at, :].astype(jnp.float32) - scale * (
            total[at, :] * kept_ref[0, r : r + 1, :]
        )
    row_devices, pair, halves = out_ref.shape[:3]
    lanes = 2 * edge
    slots = out_ref.shape[-1] // edge
    low = lax.broadcasted_iota(jnp.int32, (edge, lanes), 1) < edge
    for dest in range(row_devices):
        for e in range(halves):
            row = order[dest * halves + e]
            at = pl.ds(pl.multiple_of(row * edge, edge), edge)
            for h in range(pair):
                late = (residues[h] < row).astype(jnp.int32)
                for w in range(slots // 2):
                    start = pl.multiple_of((late + 2 * w) * lanes, lanes)
                    one = total[at, pl.ds(start, lanes)]
                    two = total[at, pl.ds(pl.multiple_of(start + lanes, lanes), lanes)]
                    if h == 0:
                        two = pltpu.roll(two, edge, 1)
                    else:
                        one = pltpu.roll(one, edge, 1)
                    out_ref[dest, h, e, 0, :, w * lanes : (w + 1) * lanes] = jnp.where(
                        low, one, two
                    ).astype(out_ref.dtype)


def step_tiles(left, tiles, own, kept, residues, order, row_devices, scale):
    groups, octet, wide = left.shape
    narrow = tiles.shape[-1]
    count = kept.shape[1]
    edge = octet // count
    halves = count // row_devices
    out = (row_devices, 2, halves, groups, edge, 4 * edge)
    return pl.pallas_call(
        functools.partial(step_kernel, scale),
        out_shape=jax.ShapeDtypeStruct(out, tiles.dtype),
        grid_spec=pltpu.PrefetchScalarGridSpec(
            num_scalar_prefetch=2,
            grid=(groups,),
            in_specs=[
                pl.BlockSpec((1, octet, wide), lambda g, *_: (g, 0, 0)),
                pl.BlockSpec(tiles.shape, lambda g, *_: (0, 0, 0)),
                pl.BlockSpec((1, octet, narrow), lambda g, *_: (g + 2, 0, 0)),
                pl.BlockSpec((1,) + kept.shape[1:], lambda g, *_: (g, 0, 0)),
            ],
            out_specs=pl.BlockSpec(
                out[:3] + (1,) + out[4:], lambda g, *_: (0, 0, 0, g, 0, 0)
            ),
            scratch_shapes=[pltpu.VMEM((octet, narrow), jnp.float32)],
        ),
        compiler_params=pltpu.CompilerParams(dimension_semantics=("arbitrary",)),
        name="step_tiles",
    )(residues, order, left, tiles, own, kept)


def deliver_kernel(panels, packed, out, send, recv, local):
    place = Place(panels)
    row_devices, pair = packed.shape[:2]
    supers = out.shape[0]
    row, col = lax.axis_index("row"), lax.axis_index("col")
    owner = place.level // 2
    sources = []
    for ring in range(supers):
        half, step = ring // place.depth, ring % place.depth
        level = step if half == 0 else place.depth - 1 - step
        sources.append((2 * half + owner, 2 * level + place.lane))
    targets = [
        (dest, 2 * (2 * place.core + h) + place.lane)
        for dest in range(row_devices)
        for h in range(pair)
    ]
    barrier = pltpu.get_barrier_semaphore()
    for source in sources:

        @pl.when(jnp.logical_or(source[0] != row, source[1] != col))
        def _(source=source):
            pl.semaphore_signal(barrier, inc=1, device_id=source, device_id_type=MESH)

    own = place.level // 2 == place.core
    pl.semaphore_wait(barrier, jnp.where(own, len(targets) - 1, len(targets)))

    def each(act_remote, act_local):
        for n, target in enumerate(targets):
            here = jnp.logical_and(target[0] == row, target[1] == col)
            dest, h = n // pair, n % pair

            @pl.when(here)
            def _(dest=dest, h=h):
                act_local(
                    pltpu.make_async_copy(packed.at[dest, h], out.at[place.ring], local)
                )

            @pl.when(jnp.logical_not(here))
            def _(dest=dest, h=h, n=n, target=target):
                act_remote(
                    remote(
                        packed.at[dest, h],
                        out.at[place.ring],
                        send.at[n],
                        recv.at[place.ring],
                        target,
                    )
                )

    each(lambda c: c.start(), lambda c: c.start())
    for n, source in enumerate(sources):

        @pl.when(jnp.logical_or(source[0] != row, source[1] != col))
        def _(n=n, source=source):
            remote(packed.at[0, 0], out.at[n], send.at[0], recv.at[n], source).wait_recv()

    each(lambda c: c.wait_send(), lambda c: c.wait())


def deliver(packed, panels, supers):
    return pl.pallas_call(
        functools.partial(deliver_kernel, panels),
        out_shape=jax.ShapeDtypeStruct((supers,) + packed.shape[2:], packed.dtype),
        in_specs=[ANY],
        out_specs=ANY,
        scratch_shapes=[
            pltpu.SemaphoreType.DMA((packed.shape[0] * packed.shape[1],)),
            pltpu.SemaphoreType.DMA((supers,)),
            pltpu.SemaphoreType.DMA,
        ],
        compiler_params=pltpu.CompilerParams(collective_id=3, has_side_effects=True),
        name="deliver",
    )(packed)


def place_kernel(inside, source, late, parts_ref, out_ref):
    supers, halves, groups, edge, width = parts_ref.shape
    count = supers * groups
    lanes = 2 * edge
    rows = out_ref.shape[0] // edge
    half = lax.broadcasted_iota(jnp.int32, (edge, lanes), 1) // edge
    first = pl.program_id(0) * rows
    e = first // count
    out_ref[...] = jnp.zeros_like(out_ref)

    @pl.loop(0, rows)
    def _(n):
        origin = source[lax.rem(first + n, count)]
        at = pl.ds(pl.multiple_of(n * edge, edge), edge)
        base = origin - 2 + late[e] + count
        for w in range(width // lanes):
            tile = parts_ref[
                origin // groups, e, lax.rem(origin, groups), :, w * lanes : (w + 1) * lanes
            ].astype(jnp.float32)
            rolled = pltpu.roll(tile, edge, 1)
            for side in range(2):
                block = inside[lax.rem(base + 2 * w + side, count)]
                odd = lax.rem(block, 2)
                value = jnp.where(odd == side, tile, rolled)
                value = jnp.where(half == odd, value, 0.0).astype(out_ref.dtype)
                to = pl.ds(pl.multiple_of((block // 2) * lanes, lanes), lanes)
                out_ref[at, to] += value


def place_blocks(parts, inside, source, late):
    supers, halves, groups, edge, width = parts.shape
    count = supers * groups
    rows = min(count, 8)
    return pl.pallas_call(
        place_kernel,
        out_shape=jax.ShapeDtypeStruct((halves * count * edge, count * edge), parts.dtype),
        grid_spec=pltpu.PrefetchScalarGridSpec(
            num_scalar_prefetch=3,
            grid=(halves * count // rows,),
            in_specs=[pl.BlockSpec(parts.shape, lambda g, *_: (0, 0, 0, 0, 0))],
            out_specs=pl.BlockSpec((rows * edge, count * edge), lambda g, *_: (g, 0)),
        ),
        compiler_params=pltpu.CompilerParams(dimension_semantics=("arbitrary",)),
        name="place_blocks",
    )(inside, source, late, parts)


def band_shards(x_vals, occupancy, perm):
    row_devices = lax.axis_size("row")
    panels = lax.axis_size("col")
    own_row, own_col = lax.axis_index("row"), lax.axis_index("col")
    count, band, area = x_vals.shape
    block_count = perm.shape[0]
    panel_cols = block_count // panels
    halves = panels // row_devices
    edge = BLOCK_EDGE
    wide = band + count

    ids = jnp.arange(panels, dtype=jnp.int32)
    spots = perm[:panels] // panel_cols
    order = jnp.sum(jnp.where(spots[None, :] == ids[:, None], ids[None, :], 0), axis=1)
    order = order.astype(jnp.int32)
    inside = (perm[::panels] % panel_cols).astype(jnp.int32)
    m_ids = jnp.arange(panel_cols, dtype=jnp.int32)
    source = jnp.sum(
        jnp.where(inside[None, :] == m_ids[:, None], m_ids[None, :], 0), axis=1
    ).astype(jnp.int32)
    lane, core = own_col % 2, own_row % 2
    mine = jnp.arange(2, dtype=jnp.int32)
    residues = order[2 * (2 * core + mine) + lane]
    late = (
        order[own_col] < lax.dynamic_slice_in_dim(order, own_row * halves, halves)
    ).astype(jnp.int32)

    lane_ids = jnp.arange(2 * edge, dtype=jnp.int32)
    wanted = jnp.where(lane_ids < edge, residues[0], residues[1]) * edge + lane_ids % edge
    pick = (jnp.arange(panels * edge, dtype=jnp.int32)[:, None] == wanted[None, :]).astype(
        x_vals.dtype
    )
    present = occupancy == 1
    rows = jnp.where(present[:, :, None], x_vals, jnp.zeros((), x_vals.dtype))
    rows = (
        rows.reshape(count, band, edge, edge)
        .transpose(0, 2, 1, 3)
        .reshape(count, edge, band * edge)
    )
    spot = jnp.arange(wide, dtype=jnp.int32)[None, :] - jnp.arange(count, dtype=jnp.int32)[:, None]
    hit = spot[:, :, None] == jnp.arange(band, dtype=jnp.int32)
    marks = jnp.any(hit & present[:, None, :], axis=2)
    marks = jnp.repeat(marks.astype(x_vals.dtype), edge, axis=1)

    all_rows, all_marks = gather_groups(rows, marks, panels)
    left, tiles, kept = lay_out(all_rows, all_marks, pick)
    tiles = exchange_halo(tiles, panels, 1)
    square = exchange_halo(square_tiles(left, tiles, kept), panels, 2)
    packed = step_tiles(
        left, square, tiles, kept, residues, order, row_devices, 0.5 / (edge * band)
    )
    parts = deliver(packed, panels, block_count // (4 * count))
    return place_blocks(parts, inside, source, late)


def shards(x_vals, occupancy, perm):
    row_devices = lax.axis_size("row")
    panels = lax.axis_size("col")
    count, band, _ = x_vals.shape
    if row_devices == 4 and panels == count == 2 * row_devices and band == 4 * count:
        return band_shards(x_vals, occupancy, perm)
    return panel_shards(x_vals, occupancy, perm)


def solution(mesh):
    return jax.shard_map(
        shards,
        mesh=mesh,
        in_specs=(P(("row", "col"), None, None), P(("row", "col"), None), P()),
        out_specs=P("row", "col"),
        check_vma=False,
    )
```

```python
import functools

import jax
import jax.numpy as jnp
from jax import lax
from jax.experimental import pallas as pl
from jax.experimental.pallas import tpu as pltpu
from jax.sharding import PartitionSpec as P

BLOCK_EDGE = 64
MESH = pl.DeviceIdType.MESH
ANY = pl.BlockSpec(memory_space=pl.ANY)


def multiply_kernel(order_ref, left_ref, far0, far1, far2, far3, out_ref):
    width = out_ref.shape[-1]
    left = left_ref[...].reshape(-1, width)
    right = jnp.concatenate([r[...].reshape(-1, width) for r in (far0, far1, far2, far3)], axis=0)
    update = jnp.dot(left, right, preferred_element_type=jnp.float32).reshape(out_ref.shape)

    @pl.when(pl.program_id(1) == 0)
    def _():
        out_ref[...] = update

    @pl.when(pl.program_id(1) != 0)
    def _():
        out_ref[...] += update


def banded_product(left, far, order, residue_major, slots):
    panels, halves, count, edge, width = left.shape
    chunk = slots // 2
    chunks = count // chunk

    def far_spec(position):
        def chunk_of(g):
            return lax.rem(2 * g + chunks - 1 + lax.rem(position + 1 + 2 * g, 4), chunks)

        if residue_major:
            return pl.BlockSpec(
                (1, chunk, edge, width), lambda g, p, order: (order[p], chunk_of(g), 0, 0)
            )
        return pl.BlockSpec(
            (chunk, 1, edge, width), lambda g, p, order: (chunk_of(g), order[p], 0, 0)
        )

    return pl.pallas_call(
        multiply_kernel,
        out_shape=jax.ShapeDtypeStruct((halves, count, edge, width), jnp.float32),
        grid_spec=pltpu.PrefetchScalarGridSpec(
            num_scalar_prefetch=1,
            grid=(count // slots, panels),
            in_specs=[
                pl.BlockSpec(
                    (1, halves, slots, edge, width), lambda g, p, order: (p, 0, g, 0, 0)
                )
            ]
            + [far_spec(position) for position in range(4)],
            out_specs=pl.BlockSpec((halves, slots, edge, width), lambda g, p, order: (0, g, 0, 0)),
        ),
        compiler_params=pltpu.CompilerParams(dimension_semantics=("arbitrary", "arbitrary")),
    )(order, left, far, far, far, far)


def spread_kernel(source_ref, target_ref, rows_ref, out_ref):
    slots = rows_ref.shape[-1] // BLOCK_EDGE
    q, n = pl.program_id(0), pl.program_id(1)
    row = q * pl.num_programs(1) + source_ref[n]
    out_ref[...] = jnp.zeros_like(out_ref)
    for v in range(slots):
        block = rows_ref[0, 0, :, v * BLOCK_EDGE : (v + 1) * BLOCK_EDGE].astype(jnp.float32)
        target = target_ref[row * slots + v]
        odd = lax.rem(target, 2)
        pair = jnp.concatenate(
            [block * (1 - odd).astype(jnp.float32), block * odd.astype(jnp.float32)], axis=1
        ).astype(out_ref.dtype)
        at = pl.multiple_of((target // 2) * (2 * BLOCK_EDGE), 2 * BLOCK_EDGE)
        out_ref[:, pl.ds(at, 2 * BLOCK_EDGE)] += pair


def spread(rows, source, target, panel_cols):
    halves, count, edge, width = rows.shape
    return pl.pallas_call(
        spread_kernel,
        out_shape=jax.ShapeDtypeStruct((halves * count * edge, panel_cols * edge), rows.dtype),
        grid_spec=pltpu.PrefetchScalarGridSpec(
            num_scalar_prefetch=2,
            grid=(halves, count),
            in_specs=[
                pl.BlockSpec((1, 1, edge, width), lambda q, n, source, target: (q, source[n], 0, 0))
            ],
            out_specs=pl.BlockSpec(
                (edge, panel_cols * edge), lambda q, n, source, target: (q * count + n, 0)
            ),
        ),
        compiler_params=pltpu.CompilerParams(dimension_semantics=("arbitrary", "arbitrary")),
    )(source, target, rows)


def band_index(m, row_residue, col_residue, slots):
    first = m - slots // 2 + (col_residue < row_residue).astype(jnp.int32)
    v = jnp.arange(slots, dtype=jnp.int32)
    first = first[..., None]
    return first + (v - first) % slots


def widen(values, index, slots):
    high = (index % (2 * slots)) >= slots
    high = jnp.repeat(high, BLOCK_EDGE, axis=-1)[..., None, :]
    zero = jnp.zeros((), values.dtype)
    return jnp.concatenate(
        [jnp.where(high, zero, values), jnp.where(high, values, zero)], axis=-1
    )


def panel_shards(x_vals, occupancy, perm):
    row_devices = lax.axis_size("row")
    panels = lax.axis_size("col")
    own_row = lax.axis_index("row")
    own_col = lax.axis_index("col")
    local_rows, band_extent, block_area = x_vals.shape
    block_count = perm.shape[0]
    panel_cols = block_count // panels
    halves = panels // row_devices
    slots = band_extent // panels
    lanes = slots * BLOCK_EDGE

    panel_of_residue = perm[:panels] // panel_cols
    residue_ids = jnp.arange(panels, dtype=jnp.int32)
    order = jnp.sum(
        jnp.where(panel_of_residue[None, :] == residue_ids[:, None], residue_ids[None, :], 0), axis=1
    ).astype(jnp.int32)
    inside = perm[::panels] % panel_cols
    m_ids = jnp.arange(panel_cols, dtype=jnp.int32)
    source = jnp.sum(
        jnp.where(inside[None, :] == m_ids[:, None], m_ids[None, :], 0), axis=1
    ).astype(jnp.int32)
    own_residue = order[own_col]
    row_residues = lax.dynamic_slice_in_dim(order, own_row * halves, halves)

    first_row = (own_row * panels + own_col) * local_rows
    row_ids = first_row + jnp.arange(local_rows, dtype=jnp.int32)
    cols = (
        row_ids[:, None] - band_extent // 2 + jnp.arange(band_extent, dtype=jnp.int32)[None, :]
    ) % block_count
    placed = (
        (occupancy[:, :, None, None] == 1)
        & ((cols % panels)[:, :, None, None] == order[None, None, :, None])
        & (
            ((cols // panels) % slots)[:, :, None, None]
            == jnp.arange(slots, dtype=jnp.int32)[None, None, None, :]
        )
    ).astype(jnp.bfloat16)
    kept = jnp.sum(placed.astype(jnp.float32), axis=1).astype(jnp.bfloat16)
    every_kept = lax.all_gather(
        kept.reshape(local_rows, panels * slots), ("row", "col"), axis=0, tiled=True
    ).reshape(panel_cols, panels, panels, slots)
    values = jnp.einsum(
        "kspt,ksf->pktf", placed, x_vals, preferred_element_type=jnp.float32
    ).astype(jnp.bfloat16)
    values = (
        values.reshape(panels, local_rows, slots, BLOCK_EDGE, BLOCK_EDGE)
        .transpose(0, 1, 3, 2, 4)
        .reshape(panels, local_rows, BLOCK_EDGE, lanes)
    )
    first = lax.all_to_all(values, "col", split_axis=0, concat_axis=0, tiled=True)
    first = first.reshape(panels * local_rows, BLOCK_EDGE, lanes)
    far = lax.all_gather(first, "row", axis=0, tiled=True).reshape(
        panel_cols, panels, BLOCK_EDGE, lanes
    )
    tile = jnp.stack(
        [
            lax.dynamic_index_in_dim(far, row_residues[q], axis=1, keepdims=False)
            for q in range(halves)
        ]
    )
    own_kept = lax.dynamic_index_in_dim(every_kept, own_col, axis=2, keepdims=False)
    wanted = jnp.stack(
        [
            lax.dynamic_index_in_dim(own_kept, row_residues[q], axis=1, keepdims=False)
            for q in range(halves)
        ]
    )
    wanted = wanted > 0
    left = lax.all_gather(tile[None], "col", axis=0, tiled=True)

    far_index = band_index(m_ids[:, None], residue_ids[None, :], own_residue, slots)
    far_wide = widen(far, far_index, slots)
    left_index = band_index(
        m_ids[None, None, :], row_residues[None, :, None], order[:, None, None], slots
    )
    left_wide = widen(left, left_index, slots)
    tile_index = band_index(m_ids[None, :], row_residues[:, None], own_residue, slots)
    tile_high = (tile_index % (2 * slots)) >= slots

    def spread_mask(mask):
        return jnp.repeat(mask, BLOCK_EDGE, axis=-1)[:, :, None, :]

    def narrow(wide):
        chosen = jnp.where(spread_mask(tile_high), wide[..., lanes:], wide[..., :lanes])
        return jnp.where(spread_mask(wanted), chosen, 0.0)

    square = narrow(banded_product(left_wide, far_wide, order, False, slots)).astype(jnp.bfloat16)
    far_square = lax.all_gather(square, "row", axis=0, tiled=True)
    square_index = band_index(m_ids[None, :], order[:, None], own_residue, slots)
    square_wide = widen(far_square, square_index, slots)
    cube = narrow(banded_product(left_wide, square_wide, residue_ids, True, slots))
    stepped = (
        1.5 * tile.astype(jnp.float32) - 0.5 / (BLOCK_EDGE * band_extent) * cube
    ).astype(jnp.bfloat16)
    hit = (tile_index % panel_cols)[..., None] == m_ids
    target = jnp.sum(jnp.where(hit, inside, 0), axis=-1).astype(jnp.int32).reshape(-1)
    return spread(stepped, source, target, panel_cols)


class Place:
    def __init__(self, panels):
        self.depth = panels // 2
        self.quarter = panels // 4
        row, col = lax.axis_index("row"), lax.axis_index("col")
        self.half, self.core = row // 2, row % 2
        self.level, self.lane = col // 2, col % 2
        self.step = jnp.where(self.half == 0, self.level, self.depth - 1 - self.level)
        self.ring = self.half * self.depth + self.step

    def device(self, half, core, level, lane):
        return (2 * half + core, 2 * level + lane)

    def at_ring(self, ring):
        half = ring // self.depth
        step = ring % self.depth
        level = jnp.where(half == 0, step, self.depth - 1 - step)
        return self.device(half, self.core, level, self.lane)

    def neighbour(self, by):
        return self.at_ring((self.ring + by + 2 * self.depth) % (2 * self.depth))

    def group_target(self):
        step = self.core * self.quarter + self.level // 2
        level = jnp.where(self.half == 0, step, self.depth - 1 - step)
        return self.device(self.half, 1 - self.level % 2, level, self.lane)

    def group_source(self):
        level = 2 * (self.step % self.quarter) + 1 - self.core
        return self.device(self.half, self.step // self.quarter, level, self.lane)


def remote(source, target, send, recv, device):
    return pltpu.make_async_remote_copy(
        src_ref=source,
        dst_ref=target,
        send_sem=send,
        recv_sem=recv,
        device_id=device,
        device_id_type=MESH,
    )


def residue_of(perm, panels, panel_cols, spot):
    found = jnp.int32(0)
    for n in range(panels):
        found = found + jnp.where(perm[n] // panel_cols == spot, n, 0)
    return found


def relayout_kernel(
    panels, spots, present, perm, x_ref, marks_in,
    out_ref, marks_ref, pick_ref, sort_ref, late_ref, mid, wide,
):
    t = pl.program_id(0)
    band, area = x_ref.shape[1:]
    edge = out_ref.shape[1]
    lanes = 2 * edge
    pairs = area // lanes
    pitch = mid.shape[0] // pairs
    low = lax.broadcasted_iota(jnp.int32, (pairs, lanes), 1) < edge

    @pl.when(t == 0)
    def _():
        marks = marks_in[...]
        count = marks.shape[0]
        left = jnp.concatenate([marks.astype(jnp.float32)] * count, axis=1)
        at = (count, count * band)
        own = lax.broadcasted_iota(jnp.int32, at, 1) // band == lax.broadcasted_iota(
            jnp.int32, at, 0
        )
        to = (count * band, marks_ref.shape[1])
        entry, lane = (lax.broadcasted_iota(jnp.int32, to, n) for n in range(2))
        right = (lane // edge - entry // band == entry % band).astype(jnp.float32)
        marks_ref[...] = jnp.dot(
            jnp.where(own, left, 0.0).astype(jnp.bfloat16),
            right.astype(jnp.bfloat16),
            preferred_element_type=jnp.float32,
        ).astype(marks_ref.dtype)
        panel_cols = perm.shape[0] // panels
        first = 4 * (lax.axis_index("row") % 2) + lax.axis_index("col") % 2
        residues = [residue_of(perm, panels, panel_cols, first + 2 * h) for h in range(2)]
        entry, lane = (lax.broadcasted_iota(jnp.int32, pick_ref.shape, n) for n in range(2))
        base = jnp.where(lane < edge, residues[0] * edge, (residues[1] - 1) * edge)
        pick_ref[...] = (entry == base + lane).astype(jnp.float32).astype(pick_ref.dtype)
        lane = lax.broadcasted_iota(jnp.int32, (1, lanes), 1)
        own = jnp.where(lane < edge, residues[0], residues[1])
        to, entry = (
            lax.broadcasted_iota(jnp.int32, (edge, sort_ref.shape[1]), n) for n in range(2)
        )
        for n in range(spots):
            spot = residue_of(perm, panels, panel_cols, n)
            sort_ref[n * edge : (n + 1) * edge, :] = (
                (entry == to + spot * edge).astype(jnp.float32).astype(sort_ref.dtype)
            )
            late_ref[n : n + 1, :] = (own < spot).astype(jnp.float32)

    for p in range(pairs):
        mid[p * pitch : p * pitch + band, :] = x_ref[
            0, :, p * lanes : (p + 1) * lanes
        ].astype(jnp.float32)
    for w in range(band // 2):
        one = mid[pl.ds(2 * w, pairs, stride=pitch), :]
        two = mid[pl.ds(2 * w + 1, pairs, stride=pitch), :]
        one = jnp.where(present[t, 2 * w] == 1, one, 0.0)
        two = jnp.where(present[t, 2 * w + 1] == 1, two, 0.0)
        wide[w, pl.ds(0, pairs, stride=2), :] = jnp.where(low, one, pltpu.roll(two, edge, 1))
        wide[w, pl.ds(1, pairs, stride=2), :] = jnp.where(low, pltpu.roll(one, edge, 1), two)
    for w in range(band // 2):
        out_ref[0, :, w * lanes : (w + 1) * lanes] = wide[w].astype(out_ref.dtype)


def relayout(x_vals, occupancy, perm, panels, edge):
    count, band, area = x_vals.shape
    lanes = 2 * edge
    octet = count * edge
    return pl.pallas_call(
        functools.partial(relayout_kernel, panels, count),
        out_shape=(
            jax.ShapeDtypeStruct((count, edge, band * edge), x_vals.dtype),
            jax.ShapeDtypeStruct((count, (band + count) * edge), x_vals.dtype),
            jax.ShapeDtypeStruct((octet, lanes), x_vals.dtype),
            jax.ShapeDtypeStruct((octet, octet), x_vals.dtype),
            jax.ShapeDtypeStruct((count, lanes), jnp.float32),
        ),
        grid_spec=pltpu.PrefetchScalarGridSpec(
            num_scalar_prefetch=2,
            grid=(count,),
            in_specs=[
                pl.BlockSpec((1, band, area), lambda t, *_: (t, 0, 0)),
                pl.BlockSpec((count, band), lambda t, *_: (0, 0)),
            ],
            out_specs=(
                pl.BlockSpec((1, edge, band * edge), lambda t, *_: (t, 0, 0)),
                pl.BlockSpec((count, (band + count) * edge), lambda t, *_: (0, 0)),
                pl.BlockSpec((octet, lanes), lambda t, *_: (0, 0)),
                pl.BlockSpec((octet, octet), lambda t, *_: (0, 0)),
                pl.BlockSpec((count, lanes), lambda t, *_: (0, 0)),
            ),
            scratch_shapes=[
                pltpu.VMEM((area // lanes * (band + 8), lanes), jnp.float32),
                pltpu.VMEM((band // 2, edge, lanes), jnp.float32),
            ],
        ),
        compiler_params=pltpu.CompilerParams(dimension_semantics=("arbitrary",)),
        name="relayout",
    )(occupancy, perm, x_vals, occupancy)


def core_kernel(
    panels, scale, rows, marks, pick, sort, late, out,
    all_rows, all_marks, left, tiles, square, kept, total, sorted_rows, packed,
    move_sems, lane_sems, core_sems, relay_sems, halo_sems, square_sems, send, recv, local,
):
    place = Place(panels)
    row, col = lax.axis_index("row"), lax.axis_index("col")
    count, edge, band_lanes = rows.shape
    octet = count * edge
    groups = all_rows.shape[0]
    wide, narrow = left.shape[-1], tiles.shape[-1]
    width = pick.shape[1]
    row_devices, pair = packed.shape[:2]
    halves = packed.shape[3]
    supers = out.shape[0]

    target, source = place.group_target(), place.group_source()
    lane_peer = place.device(place.half, place.core, place.level, 1 - place.lane)
    core_peer = place.device(place.half, 1 - place.core, place.level, place.lane)
    after, before = place.neighbour(1), place.neighbour(-1)
    target_slot = 2 * (place.level % 2) + place.lane
    own_slot = 2 * (1 - place.core) + place.lane
    peer_slot = 2 * (1 - place.core) + 1 - place.lane
    third_slot = 2 * place.core + place.lane
    last_slot = 2 * place.core + 1 - place.lane
    owner = place.level // 2
    senders = []
    for ring in range(supers):
        half, step = ring // place.depth, ring % place.depth
        level = step if half == 0 else place.depth - 1 - step
        senders.append((2 * half + owner, 2 * level + place.lane))
    receivers = [
        (dest, 2 * (2 * place.core + h) + place.lane)
        for dest in range(row_devices)
        for h in range(pair)
    ]

    def is_here(device):
        return jnp.logical_and(device[0] == row, device[1] == col)

    barrier = pltpu.get_barrier_semaphore()
    for device in (source, lane_peer, core_peer, after, before):
        pl.semaphore_signal(barrier, inc=1, device_id=device, device_id_type=MESH)
    for device in senders:

        @pl.when(jnp.logical_not(is_here(device)))
        def _(device=device):
            pl.semaphore_signal(barrier, inc=1, device_id=device, device_id_type=MESH)

    expected = 5 + len(receivers)
    pl.semaphore_wait(barrier, jnp.where(owner == place.core, expected - 1, expected))

    def copy_of(n, sems, device, slot, first=False):
        origin = rows.at[n] if first else all_rows.at[slot, n]
        return remote(origin, all_rows.at[slot, n], sems.at[0, n], sems.at[1, n], device)

    def mark_of(sems, device, slot, first=False):
        origin = marks if first else all_marks.at[slot]
        return remote(
            origin, all_marks.at[slot], sems.at[0, count], sems.at[1, count], device
        )

    mark_copies = [
        mark_of(move_sems, target, target_slot, True),
        mark_of(lane_sems, lane_peer, own_slot),
        mark_of(core_sems, core_peer, own_slot),
        mark_of(relay_sems, core_peer, peer_slot),
    ]
    mark_copies[0].start()

    @pl.loop(0, count)
    def _(n):
        copy_of(n, move_sems, target, target_slot, True).start()

    @pl.loop(0, groups)
    def _(t):
        left[t] = jnp.zeros(left.shape[1:], left.dtype)

    def lay(slot, m):
        base = pl.multiple_of(2 * m * edge, 2 * edge)
        zeros = jnp.zeros((edge, edge), left.dtype)
        reach = pl.ds(base, band_lanes + 2 * edge)
        left[slot, pl.ds(base, edge), pl.ds(base, band_lanes)] = all_rows[slot, 2 * m]
        left[slot, pl.ds(pl.multiple_of(base + edge, edge), edge), reach] = jnp.concatenate(
            [zeros, all_rows[slot, 2 * m + 1], zeros], axis=1
        )
        chosen = pick[...]
        for o in range(wide // octet):
            tiles[slot + 2, pl.ds(base, 2 * edge), o * width : (o + 1) * width] = jnp.dot(
                left[slot, pl.ds(base, 2 * edge), o * octet : (o + 1) * octet],
                chosen,
                preferred_element_type=jnp.float32,
            ).astype(tiles.dtype)

    mark_copies[0].wait_recv()
    mark_copies[1].start()
    mark_copies[2].start()

    @pl.loop(0, count // 2)
    def _(m):
        for n in (2 * m, 2 * m + 1):
            copy_of(n, move_sems, target, target_slot, True).wait_recv()
            copy_of(n, lane_sems, lane_peer, own_slot).start()
            copy_of(n, core_sems, core_peer, own_slot).start()
        lay(own_slot, m)
        for n in (2 * m, 2 * m + 1):
            copy_of(n, lane_sems, lane_peer, own_slot).wait_recv()
            copy_of(n, relay_sems, core_peer, peer_slot).start()
        lay(peer_slot, m)
        for n in (2 * m, 2 * m + 1):
            copy_of(n, core_sems, core_peer, own_slot).wait_recv()
        lay(third_slot, m)
        for n in (2 * m, 2 * m + 1):
            copy_of(n, relay_sems, core_peer, peer_slot).wait_recv()
        lay(last_slot, m)

    def halo(ref, sems):
        step = narrow // 5
        moves = (
            (groups + 1, 1, slice(step, narrow), after),
            (groups, 0, slice(2 * step, narrow), after),
            (2, groups + 2, slice(0, 4 * step), before),
            (3, groups + 3, slice(0, 3 * step), before),
        )
        return [
            remote(
                ref.at[origin, :, lanes], ref.at[to, :, lanes], sems.at[0, n], sems.at[1, n], device
            )
            for n, (origin, to, lanes, device) in enumerate(moves)
        ]

    first_halo = halo(tiles, halo_sems)
    for copy in first_halo:
        copy.start()

    mark_copies[1].wait_recv()
    mark_copies[3].start()
    mark_copies[2].wait_recv()
    mark_copies[3].wait_recv()
    for t in range(groups):
        for o in range(wide // octet):
            kept[t, :, o * width : (o + 1) * width] = jnp.dot(
                all_marks[t, :, o * octet : (o + 1) * octet],
                pick[...],
                preferred_element_type=jnp.float32,
            )

    def term(ref, t, by, fresh=False):
        step = narrow // 5
        reach = narrow - abs(by) * step
        first = 0 if by >= 0 else narrow - reach
        to = max(by, 0) * step
        update = jnp.dot(
            left[t, :, (2 + by) * octet : (3 + by) * octet],
            ref[t + 2 + by, :, first : first + reach],
            preferred_element_type=jnp.float32,
        )
        if fresh:
            total[t] = update
        else:
            total[t, :, to : to + reach] += update

    def own_terms(ref):
        @pl.loop(0, groups)
        def _(t):
            term(ref, t, 0, True)
            for by in (-2, -1, 1, 2):

                @pl.when(jnp.logical_and(t + by >= 0, t + by < groups))
                def _(by=by):
                    term(ref, t, by)

    def halo_terms(ref, t):
        for by in (-2, -1, 1, 2):
            if not 0 <= t + by < groups:
                term(ref, t, by)

    own_terms(tiles)
    second_halo = halo(square, square_sems)
    waits = {1: (0,), 0: (1,), 2: (2,), 3: (3,)}
    sends = {1: 3, 0: 2, 2: 1, 3: 0}
    for t in (1, 0, 2, 3):
        for n in waits[t]:
            first_halo[n].wait_recv()
        halo_terms(tiles, t)
        for r in range(count):
            at = slice(r * edge, (r + 1) * edge)
            square[t + 2, at, :] = (total[t, at, :] * kept[t, r : r + 1, :]).astype(square.dtype)
        second_halo[{1: 3, 0: 2, 2: 1, 3: 0}[t]].start()

    own_terms(square)
    lanes = 2 * edge
    low = lax.broadcasted_iota(jnp.int32, (edge, lanes), 1) < edge

    def delivery(t, n):
        dest, h = n // pair, n % pair
        return remote(
            packed.at[dest, h, t],
            out.at[place.ring, t],
            send.at[n, t],
            recv.at[place.ring, t],
            receivers[n],
        )

    def kept_here(t, n):
        return pltpu.make_async_copy(
            packed.at[n // pair, n % pair, t], out.at[place.ring, t], local.at[t]
        )

    def each_receiver(t, away, here):
        for n, device in enumerate(receivers):

            @pl.when(is_here(device))
            def _(n=n):
                here(kept_here(t, n))

            @pl.when(jnp.logical_not(is_here(device)))
            def _(n=n):
                away(delivery(t, n))

    for t in (1, 0, 2, 3):
        for n in waits[t]:
            second_halo[n].wait_recv()
        halo_terms(square, t)
        for r in range(count):
            at = slice(r * edge, (r + 1) * edge)
            total[t, at, :] = 1.5 * tiles[t + 2, at, :].astype(jnp.float32) - scale * (
                total[t, at, :] * kept[t, r : r + 1, :]
            )
        sorted_rows[...] = jnp.dot(
            sort[...], total[t].astype(packed.dtype), preferred_element_type=jnp.float32
        )
        for n in range(row_devices * halves):
            dest, e = n // halves, n % halves
            at = slice(n * edge, (n + 1) * edge)
            shift = late[n : n + 1, :] > 0.5
            parts = [sorted_rows[at, o * lanes : (o + 1) * lanes] for o in range(narrow // lanes)]
            parts = [jnp.where(shift, two, one) for one, two in zip(parts, parts[1:])]
            turned = [pltpu.roll(part, edge, 1) for part in parts]
            for w in range(len(parts) // 2):
                to = slice(w * lanes, (w + 1) * lanes)
                packed[dest, 0, t, e, :, to] = jnp.where(
                    low, parts[2 * w], turned[2 * w + 1]
                ).astype(packed.dtype)
                packed[dest, 1, t, e, :, to] = jnp.where(
                    low, turned[2 * w], parts[2 * w + 1]
                ).astype(packed.dtype)
        each_receiver(t, lambda copy: copy.start(), lambda copy: copy.start())

    for copy in mark_copies + first_halo + second_halo:
        copy.wait_send()

    @pl.loop(0, count)
    def _(n):
        copy_of(n, move_sems, target, target_slot, True).wait_send()
        copy_of(n, lane_sems, lane_peer, own_slot).wait_send()
        copy_of(n, core_sems, core_peer, own_slot).wait_send()
        copy_of(n, relay_sems, core_peer, peer_slot).wait_send()

    for t in (1, 0, 2, 3):
        for n, device in enumerate(senders):

            @pl.when(jnp.logical_not(is_here(device)))
            def _(t=t, n=n, device=device):
                remote(
                    packed.at[0, 0, t], out.at[n, t], send.at[0, t], recv.at[n, t], device
                ).wait_recv()

        each_receiver(t, lambda copy: copy.wait_send(), lambda copy: copy.wait())


def band_step(rows, marks, pick, sort, late, row_devices, panels, block_count, scale):
    count, edge, band_lanes = rows.shape
    octet, wide = count * edge, marks.shape[-1]
    narrow = wide // octet * 2 * edge
    halves = panels // row_devices
    supers = block_count // (4 * count)
    vmem = pl.BlockSpec(memory_space=pltpu.VMEM)
    kind = rows.dtype
    out = (supers, 4, halves, edge, 4 * edge)
    dma = pltpu.SemaphoreType.DMA
    return pl.pallas_call(
        functools.partial(core_kernel, panels, scale),
        out_shape=jax.ShapeDtypeStruct(out, kind),
        in_specs=[ANY, ANY, vmem, vmem, vmem],
        out_specs=ANY,
        scratch_shapes=[
            pltpu.VMEM((4,) + rows.shape, kind),
            pltpu.VMEM((4,) + marks.shape, kind),
            pltpu.VMEM((4, octet, wide), kind),
            pltpu.VMEM((8, octet, narrow), kind),
            pltpu.VMEM((8, octet, narrow), kind),
            pltpu.VMEM((4, count, narrow), jnp.float32),
            pltpu.VMEM((4, octet, narrow), jnp.float32),
            pltpu.VMEM((octet, narrow), jnp.float32),
            pltpu.VMEM((row_devices, 2) + out[1:], kind),
            dma((2, count + 1)),
            dma((2, count + 1)),
            dma((2, count + 1)),
            dma((2, count + 1)),
            dma((2, 4)),
            dma((2, 4)),
            dma((2 * row_devices, 4)),
            dma((supers, 4)),
            dma((4,)),
        ],
        compiler_params=pltpu.CompilerParams(
            collective_id=0, has_side_effects=True, vmem_limit_bytes=60 * 2**20
        ),
        name="band_step",
    )(rows, marks, pick, sort, late)


def place_kernel(panels, perm, parts_ref, out_ref, origins):
    supers, groups, halves, edge, width = parts_ref.shape
    count = supers * groups
    lanes = 2 * edge
    rows = out_ref.shape[0] // edge
    half = lax.broadcasted_iota(jnp.int32, (edge, lanes), 1) // edge
    first = pl.program_id(0) * rows
    e = first // count

    @pl.when(first == 0)
    def _():
        @pl.loop(0, count)
        def _(n):
            origins[perm[n * panels] % count] = n

    residue = residue_of(perm, panels, count, lax.axis_index("col"))
    spot = residue_of(perm, panels, count, lax.axis_index("row") * halves + e)
    late = (residue < spot).astype(jnp.int32)
    out_ref[...] = jnp.zeros_like(out_ref)

    @pl.loop(0, rows)
    def _(n):
        origin = origins[lax.rem(first + n, count)]
        at = pl.ds(pl.multiple_of(n * edge, edge), edge)
        base = origin - 2 + late + count
        for w in range(width // lanes):
            tile = parts_ref[
                origin // groups, lax.rem(origin, groups), e, :, w * lanes : (w + 1) * lanes
            ].astype(jnp.float32)
            rolled = pltpu.roll(tile, edge, 1)
            for side in range(2):
                block = perm[lax.rem(base + 2 * w + side, count) * panels] % count
                odd = lax.rem(block, 2)
                value = jnp.where(odd == side, tile, rolled)
                value = jnp.where(half == odd, value, 0.0).astype(out_ref.dtype)
                to = pl.ds(pl.multiple_of((block // 2) * lanes, lanes), lanes)
                out_ref[at, to] += value


def place_blocks(parts, perm, panels):
    supers, groups, halves, edge, width = parts.shape
    count = supers * groups
    rows = min(count, 8)
    return pl.pallas_call(
        functools.partial(place_kernel, panels),
        out_shape=jax.ShapeDtypeStruct((halves * count * edge, count * edge), parts.dtype),
        grid_spec=pltpu.PrefetchScalarGridSpec(
            num_scalar_prefetch=1,
            grid=(halves * count // rows,),
            in_specs=[pl.BlockSpec(parts.shape, lambda g, *_: (0, 0, 0, 0, 0))],
            out_specs=pl.BlockSpec((rows * edge, count * edge), lambda g, *_: (g, 0)),
            scratch_shapes=[pltpu.SMEM((count,), jnp.int32)],
        ),
        compiler_params=pltpu.CompilerParams(dimension_semantics=("arbitrary",)),
        name="place_blocks",
    )(perm, parts)


def band_shards(x_vals, occupancy, perm):
    row_devices = lax.axis_size("row")
    panels = lax.axis_size("col")
    band = x_vals.shape[1]
    made = relayout(x_vals, occupancy, perm, panels, BLOCK_EDGE)
    scale = 0.5 / (BLOCK_EDGE * band)
    parts = band_step(*made, row_devices, panels, perm.shape[0], scale)
    return place_blocks(parts, perm, panels)


def shards(x_vals, occupancy, perm):
    row_devices = lax.axis_size("row")
    panels = lax.axis_size("col")
    count, band, _ = x_vals.shape
    if row_devices == 4 and panels == count == 2 * row_devices and band == 4 * count:
        return band_shards(x_vals, occupancy, perm)
    return panel_shards(x_vals, occupancy, perm)


def solution(mesh):
    return jax.shard_map(
        shards,
        mesh=mesh,
        in_specs=(P(("row", "col"), None, None), P(("row", "col"), None), P()),
        out_specs=P("row", "col"),
        check_vma=False,
    )
```

```python
import functools

import jax
import jax.numpy as jnp
from jax import lax
from jax.experimental import pallas as pl
from jax.experimental.pallas import tpu as pltpu
from jax.sharding import PartitionSpec as P

BLOCK_EDGE = 64
MESH = pl.DeviceIdType.MESH
ANY = pl.BlockSpec(memory_space=pl.ANY)


def multiply_kernel(order_ref, left_ref, far0, far1, far2, far3, out_ref):
    width = out_ref.shape[-1]
    left = left_ref[...].reshape(-1, width)
    right = jnp.concatenate([r[...].reshape(-1, width) for r in (far0, far1, far2, far3)], axis=0)
    update = jnp.dot(left, right, preferred_element_type=jnp.float32).reshape(out_ref.shape)

    @pl.when(pl.program_id(1) == 0)
    def _():
        out_ref[...] = update

    @pl.when(pl.program_id(1) != 0)
    def _():
        out_ref[...] += update


def banded_product(left, far, order, residue_major, slots):
    panels, halves, count, edge, width = left.shape
    chunk = slots // 2
    chunks = count // chunk

    def far_spec(position):
        def chunk_of(g):
            return lax.rem(2 * g + chunks - 1 + lax.rem(position + 1 + 2 * g, 4), chunks)

        if residue_major:
            return pl.BlockSpec(
                (1, chunk, edge, width), lambda g, p, order: (order[p], chunk_of(g), 0, 0)
            )
        return pl.BlockSpec(
            (chunk, 1, edge, width), lambda g, p, order: (chunk_of(g), order[p], 0, 0)
        )

    return pl.pallas_call(
        multiply_kernel,
        out_shape=jax.ShapeDtypeStruct((halves, count, edge, width), jnp.float32),
        grid_spec=pltpu.PrefetchScalarGridSpec(
            num_scalar_prefetch=1,
            grid=(count // slots, panels),
            in_specs=[
                pl.BlockSpec(
                    (1, halves, slots, edge, width), lambda g, p, order: (p, 0, g, 0, 0)
                )
            ]
            + [far_spec(position) for position in range(4)],
            out_specs=pl.BlockSpec((halves, slots, edge, width), lambda g, p, order: (0, g, 0, 0)),
        ),
        compiler_params=pltpu.CompilerParams(dimension_semantics=("arbitrary", "arbitrary")),
    )(order, left, far, far, far, far)


def spread_kernel(source_ref, target_ref, rows_ref, out_ref):
    slots = rows_ref.shape[-1] // BLOCK_EDGE
    q, n = pl.program_id(0), pl.program_id(1)
    row = q * pl.num_programs(1) + source_ref[n]
    out_ref[...] = jnp.zeros_like(out_ref)
    for v in range(slots):
        block = rows_ref[0, 0, :, v * BLOCK_EDGE : (v + 1) * BLOCK_EDGE].astype(jnp.float32)
        target = target_ref[row * slots + v]
        odd = lax.rem(target, 2)
        pair = jnp.concatenate(
            [block * (1 - odd).astype(jnp.float32), block * odd.astype(jnp.float32)], axis=1
        ).astype(out_ref.dtype)
        at = pl.multiple_of((target // 2) * (2 * BLOCK_EDGE), 2 * BLOCK_EDGE)
        out_ref[:, pl.ds(at, 2 * BLOCK_EDGE)] += pair


def spread(rows, source, target, panel_cols):
    halves, count, edge, width = rows.shape
    return pl.pallas_call(
        spread_kernel,
        out_shape=jax.ShapeDtypeStruct((halves * count * edge, panel_cols * edge), rows.dtype),
        grid_spec=pltpu.PrefetchScalarGridSpec(
            num_scalar_prefetch=2,
            grid=(halves, count),
            in_specs=[
                pl.BlockSpec((1, 1, edge, width), lambda q, n, source, target: (q, source[n], 0, 0))
            ],
            out_specs=pl.BlockSpec(
                (edge, panel_cols * edge), lambda q, n, source, target: (q * count + n, 0)
            ),
        ),
        compiler_params=pltpu.CompilerParams(dimension_semantics=("arbitrary", "arbitrary")),
    )(source, target, rows)


def band_index(m, row_residue, col_residue, slots):
    first = m - slots // 2 + (col_residue < row_residue).astype(jnp.int32)
    v = jnp.arange(slots, dtype=jnp.int32)
    first = first[..., None]
    return first + (v - first) % slots


def widen(values, index, slots):
    high = (index % (2 * slots)) >= slots
    high = jnp.repeat(high, BLOCK_EDGE, axis=-1)[..., None, :]
    zero = jnp.zeros((), values.dtype)
    return jnp.concatenate(
        [jnp.where(high, zero, values), jnp.where(high, values, zero)], axis=-1
    )


def panel_shards(x_vals, occupancy, perm):
    row_devices = lax.axis_size("row")
    panels = lax.axis_size("col")
    own_row = lax.axis_index("row")
    own_col = lax.axis_index("col")
    local_rows, band_extent, block_area = x_vals.shape
    block_count = perm.shape[0]
    panel_cols = block_count // panels
    halves = panels // row_devices
    slots = band_extent // panels
    lanes = slots * BLOCK_EDGE

    panel_of_residue = perm[:panels] // panel_cols
    residue_ids = jnp.arange(panels, dtype=jnp.int32)
    order = jnp.sum(
        jnp.where(panel_of_residue[None, :] == residue_ids[:, None], residue_ids[None, :], 0), axis=1
    ).astype(jnp.int32)
    inside = perm[::panels] % panel_cols
    m_ids = jnp.arange(panel_cols, dtype=jnp.int32)
    source = jnp.sum(
        jnp.where(inside[None, :] == m_ids[:, None], m_ids[None, :], 0), axis=1
    ).astype(jnp.int32)
    own_residue = order[own_col]
    row_residues = lax.dynamic_slice_in_dim(order, own_row * halves, halves)

    first_row = (own_row * panels + own_col) * local_rows
    row_ids = first_row + jnp.arange(local_rows, dtype=jnp.int32)
    cols = (
        row_ids[:, None] - band_extent // 2 + jnp.arange(band_extent, dtype=jnp.int32)[None, :]
    ) % block_count
    placed = (
        (occupancy[:, :, None, None] == 1)
        & ((cols % panels)[:, :, None, None] == order[None, None, :, None])
        & (
            ((cols // panels) % slots)[:, :, None, None]
            == jnp.arange(slots, dtype=jnp.int32)[None, None, None, :]
        )
    ).astype(jnp.bfloat16)
    kept = jnp.sum(placed.astype(jnp.float32), axis=1).astype(jnp.bfloat16)
    every_kept = lax.all_gather(
        kept.reshape(local_rows, panels * slots), ("row", "col"), axis=0, tiled=True
    ).reshape(panel_cols, panels, panels, slots)
    values = jnp.einsum(
        "kspt,ksf->pktf", placed, x_vals, preferred_element_type=jnp.float32
    ).astype(jnp.bfloat16)
    values = (
        values.reshape(panels, local_rows, slots, BLOCK_EDGE, BLOCK_EDGE)
        .transpose(0, 1, 3, 2, 4)
        .reshape(panels, local_rows, BLOCK_EDGE, lanes)
    )
    first = lax.all_to_all(values, "col", split_axis=0, concat_axis=0, tiled=True)
    first = first.reshape(panels * local_rows, BLOCK_EDGE, lanes)
    far = lax.all_gather(first, "row", axis=0, tiled=True).reshape(
        panel_cols, panels, BLOCK_EDGE, lanes
    )
    tile = jnp.stack(
        [
            lax.dynamic_index_in_dim(far, row_residues[q], axis=1, keepdims=False)
            for q in range(halves)
        ]
    )
    own_kept = lax.dynamic_index_in_dim(every_kept, own_col, axis=2, keepdims=False)
    wanted = jnp.stack(
        [
            lax.dynamic_index_in_dim(own_kept, row_residues[q], axis=1, keepdims=False)
            for q in range(halves)
        ]
    )
    wanted = wanted > 0
    left = lax.all_gather(tile[None], "col", axis=0, tiled=True)

    far_index = band_index(m_ids[:, None], residue_ids[None, :], own_residue, slots)
    far_wide = widen(far, far_index, slots)
    left_index = band_index(
        m_ids[None, None, :], row_residues[None, :, None], order[:, None, None], slots
    )
    left_wide = widen(left, left_index, slots)
    tile_index = band_index(m_ids[None, :], row_residues[:, None], own_residue, slots)
    tile_high = (tile_index % (2 * slots)) >= slots

    def spread_mask(mask):
        return jnp.repeat(mask, BLOCK_EDGE, axis=-1)[:, :, None, :]

    def narrow(wide):
        chosen = jnp.where(spread_mask(tile_high), wide[..., lanes:], wide[..., :lanes])
        return jnp.where(spread_mask(wanted), chosen, 0.0)

    square = narrow(banded_product(left_wide, far_wide, order, False, slots)).astype(jnp.bfloat16)
    far_square = lax.all_gather(square, "row", axis=0, tiled=True)
    square_index = band_index(m_ids[None, :], order[:, None], own_residue, slots)
    square_wide = widen(far_square, square_index, slots)
    cube = narrow(banded_product(left_wide, square_wide, residue_ids, True, slots))
    stepped = (
        1.5 * tile.astype(jnp.float32) - 0.5 / (BLOCK_EDGE * band_extent) * cube
    ).astype(jnp.bfloat16)
    hit = (tile_index % panel_cols)[..., None] == m_ids
    target = jnp.sum(jnp.where(hit, inside, 0), axis=-1).astype(jnp.int32).reshape(-1)
    return spread(stepped, source, target, panel_cols)


class Place:
    def __init__(self, panels):
        self.depth = panels // 2
        self.quarter = panels // 4
        row, col = lax.axis_index("row"), lax.axis_index("col")
        self.half, self.core = row // 2, row % 2
        self.level, self.lane = col // 2, col % 2
        self.step = jnp.where(self.half == 0, self.level, self.depth - 1 - self.level)
        self.ring = self.half * self.depth + self.step

    def device(self, half, core, level, lane):
        return (2 * half + core, 2 * level + lane)

    def at_ring(self, ring):
        half = ring // self.depth
        step = ring % self.depth
        level = jnp.where(half == 0, step, self.depth - 1 - step)
        return self.device(half, self.core, level, self.lane)

    def neighbour(self, by):
        return self.at_ring((self.ring + by + 2 * self.depth) % (2 * self.depth))

    def group_target(self):
        step = self.core * self.quarter + self.level // 2
        level = jnp.where(self.half == 0, step, self.depth - 1 - step)
        return self.device(self.half, 1 - self.level % 2, level, self.lane)

    def group_source(self):
        level = 2 * (self.step % self.quarter) + 1 - self.core
        return self.device(self.half, self.step // self.quarter, level, self.lane)


def remote(source, target, send, recv, device):
    return pltpu.make_async_remote_copy(
        src_ref=source,
        dst_ref=target,
        send_sem=send,
        recv_sem=recv,
        device_id=device,
        device_id_type=MESH,
    )


def residue_of(perm, panels, panel_cols, spot):
    found = jnp.int32(0)
    for n in range(panels):
        found = found + jnp.where(perm[n] // panel_cols == spot, n, 0)
    return found


def core_kernel(
    panels, scale, present, perm, x_ref, flags, out,
    rows, marks, pick, sort, late, mid, pairs,
    all_rows, all_marks, left, tiles, square, kept, total, sorted_rows, packed,
    move_sems, lane_sems, core_sems, relay_sems, halo_sems, square_sems, send, recv, local,
):
    place = Place(panels)
    row, col = lax.axis_index("row"), lax.axis_index("col")
    count, edge, band_lanes = rows.shape
    octet = count * edge
    groups = all_rows.shape[0]
    wide, narrow = left.shape[-1], tiles.shape[-1]
    width = pick.shape[1]
    row_devices, pair = packed.shape[:2]
    halves = packed.shape[3]
    supers = out.shape[0]

    target, source = place.group_target(), place.group_source()
    lane_peer = place.device(place.half, place.core, place.level, 1 - place.lane)
    core_peer = place.device(place.half, 1 - place.core, place.level, place.lane)
    after, before = place.neighbour(1), place.neighbour(-1)
    target_slot = 2 * (place.level % 2) + place.lane
    own_slot = 2 * (1 - place.core) + place.lane
    peer_slot = 2 * (1 - place.core) + 1 - place.lane
    third_slot = 2 * place.core + place.lane
    last_slot = 2 * place.core + 1 - place.lane
    owner = place.level // 2
    senders = []
    for ring in range(supers):
        half, step = ring // place.depth, ring % place.depth
        level = step if half == 0 else place.depth - 1 - step
        senders.append((2 * half + owner, 2 * level + place.lane))
    receivers = [
        (dest, 2 * (2 * place.core + h) + place.lane)
        for dest in range(row_devices)
        for h in range(pair)
    ]

    def is_here(device):
        return jnp.logical_and(device[0] == row, device[1] == col)

    barrier = pltpu.get_barrier_semaphore()
    for device in (source, lane_peer, core_peer, after, before):
        pl.semaphore_signal(barrier, inc=1, device_id=device, device_id_type=MESH)
    for device in senders:

        @pl.when(jnp.logical_not(is_here(device)))
        def _(device=device):
            pl.semaphore_signal(barrier, inc=1, device_id=device, device_id_type=MESH)

    expected = 5 + len(receivers)
    pl.semaphore_wait(barrier, jnp.where(owner == place.core, expected - 1, expected))

    def piece_of(ref, n):
        return ref.at[n // 2, pl.ds(n % 2 * (edge // 2), edge // 2)]

    def copy_of(n, sems, device, slot, first=False):
        landing = piece_of(all_rows.at[slot], n)
        origin = piece_of(rows, n) if first else landing
        return remote(origin, landing, sems.at[0, n], sems.at[1, n], device)

    def mark_of(sems, device, slot, first=False):
        origin = marks if first else all_marks.at[slot]
        return remote(
            origin, all_marks.at[slot], sems.at[0, 2 * count], sems.at[1, 2 * count], device
        )

    mark_copies = [
        mark_of(move_sems, target, target_slot, True),
        mark_of(lane_sems, lane_peer, own_slot),
        mark_of(core_sems, core_peer, own_slot),
        mark_of(relay_sems, core_peer, peer_slot),
    ]
    lanes = 2 * edge
    low = lax.broadcasted_iota(jnp.int32, (edge, lanes), 1) < edge
    panel_cols = perm.shape[0] // panels
    band, area = x_ref.shape[1:]
    tall = area // lanes
    pitch = mid.shape[0] // tall

    def relay_row(t):
        for p in range(tall):
            mid[p * pitch : p * pitch + band, :] = x_ref[
                t, :, p * lanes : (p + 1) * lanes
            ].astype(jnp.float32)
        for w in range(band // 2):
            one = mid[pl.ds(2 * w, tall, stride=pitch), :] * present[t, 2 * w].astype(jnp.float32)
            two = mid[pl.ds(2 * w + 1, tall, stride=pitch), :] * present[t, 2 * w + 1].astype(
                jnp.float32
            )
            lower = low[:tall]
            pairs[w, pl.ds(0, tall, stride=2), :] = jnp.where(
                lower, one, pltpu.roll(two, edge, 1)
            )
            pairs[w, pl.ds(1, tall, stride=2), :] = jnp.where(
                lower, pltpu.roll(one, edge, 1), two
            )
        for w in range(band // 2):
            rows[t, :, w * lanes : (w + 1) * lanes] = pairs[w].astype(rows.dtype)

    @pl.loop(0, count)
    def _(t):
        relay_row(t)

        @pl.when(t > 0)
        def _():
            for n in range(2):
                copy_of(2 * (t - 1) + n, move_sems, target, target_slot, True).start()

    wide_flags = jnp.concatenate([flags[...].astype(jnp.float32)] * count, axis=1)
    at = (count, count * band)
    own = lax.broadcasted_iota(jnp.int32, at, 1) // band == lax.broadcasted_iota(jnp.int32, at, 0)
    to = (count * band, wide)
    entry, lane = (lax.broadcasted_iota(jnp.int32, to, n) for n in range(2))
    spread = (lane // edge - entry // band == entry % band).astype(jnp.float32)
    marks[...] = jnp.dot(
        jnp.where(own, wide_flags, 0.0).astype(marks.dtype),
        spread.astype(marks.dtype),
        preferred_element_type=jnp.float32,
    ).astype(marks.dtype)
    for n in range(2):
        copy_of(2 * (count - 1) + n, move_sems, target, target_slot, True).start()
    first = 4 * place.core + place.lane
    residues = [residue_of(perm, panels, panel_cols, first + 2 * h) for h in range(2)]
    entry, lane = (lax.broadcasted_iota(jnp.int32, pick.shape, n) for n in range(2))
    base = jnp.where(lane < edge, residues[0] * edge, (residues[1] - 1) * edge)
    pick[...] = (entry == base + lane).astype(jnp.float32).astype(pick.dtype)
    mark_copies[0].start()
    lane = lax.broadcasted_iota(jnp.int32, (1, lanes), 1)
    own = jnp.where(lane < edge, residues[0], residues[1])
    to, entry = (lax.broadcasted_iota(jnp.int32, (edge, octet), n) for n in range(2))
    for n in range(row_devices * halves):
        spot = residue_of(perm, panels, panel_cols, n)
        sort[n * edge : (n + 1) * edge, :] = (
            (entry == to + spot * edge).astype(jnp.float32).astype(sort.dtype)
        )
        late[n : n + 1, :] = (own < spot).astype(jnp.float32)

    @pl.loop(0, groups)
    def _(t):
        left[t] = jnp.zeros(left.shape[1:], left.dtype)

    def lay(slot, m):
        base = pl.multiple_of(2 * m * edge, 2 * edge)
        zeros = jnp.zeros((edge, edge), left.dtype)
        reach = pl.ds(base, band_lanes + 2 * edge)
        left[slot, pl.ds(base, edge), pl.ds(base, band_lanes)] = all_rows[slot, 2 * m]
        left[slot, pl.ds(pl.multiple_of(base + edge, edge), edge), reach] = jnp.concatenate(
            [zeros, all_rows[slot, 2 * m + 1], zeros], axis=1
        )
        chosen = pick[...]
        for o in range(wide // octet):
            tiles[slot + 2, pl.ds(base, 2 * edge), o * width : (o + 1) * width] = jnp.dot(
                left[slot, pl.ds(base, 2 * edge), o * octet : (o + 1) * octet],
                chosen,
                preferred_element_type=jnp.float32,
            ).astype(tiles.dtype)

    rounds = count // 2

    @pl.loop(0, rounds + 2)
    def _(m):
        @pl.when(m < rounds)
        def _():
            for i in range(4):
                n = 4 * m + i
                copy_of(n, move_sems, target, target_slot, True).wait_recv()
                copy_of(n, lane_sems, lane_peer, own_slot).start()
                copy_of(n, core_sems, core_peer, own_slot).start()

        @pl.when(jnp.logical_and(m > 0, m <= rounds))
        def _():
            for i in range(4):
                n = 4 * (m - 1) + i
                copy_of(n, lane_sems, lane_peer, own_slot).wait_recv()
                copy_of(n, relay_sems, core_peer, peer_slot).start()

        @pl.when(m < rounds)
        def _():
            lay(own_slot, m)

        @pl.when(jnp.logical_and(m > 0, m <= rounds))
        def _():
            for i in range(4):
                copy_of(4 * (m - 1) + i, core_sems, core_peer, own_slot).wait_recv()
            lay(peer_slot, m - 1)
            lay(third_slot, m - 1)

        @pl.when(m > 1)
        def _():
            for i in range(4):
                copy_of(4 * (m - 2) + i, relay_sems, core_peer, peer_slot).wait_recv()
            lay(last_slot, m - 2)

    mark_copies[0].wait_recv()
    mark_copies[1].start()
    mark_copies[2].start()

    def halo(ref, sems):
        step = narrow // 5
        moves = (
            (groups + 1, 1, slice(step, narrow), after),
            (groups, 0, slice(2 * step, narrow), after),
            (2, groups + 2, slice(0, 4 * step), before),
            (3, groups + 3, slice(0, 3 * step), before),
        )
        return [
            remote(
                ref.at[origin, :, lanes], ref.at[to, :, lanes], sems.at[0, n], sems.at[1, n], device
            )
            for n, (origin, to, lanes, device) in enumerate(moves)
        ]

    first_halo = halo(tiles, halo_sems)
    for copy in first_halo:
        copy.start()

    mark_copies[1].wait_recv()
    mark_copies[3].start()
    mark_copies[2].wait_recv()
    mark_copies[3].wait_recv()
    for t in range(groups):
        for o in range(wide // octet):
            kept[t, :, o * width : (o + 1) * width] = jnp.dot(
                all_marks[t, :, o * octet : (o + 1) * octet],
                pick[...],
                preferred_element_type=jnp.float32,
            )

    def term(ref, t, by, fresh=False):
        step = narrow // 5
        reach = narrow - abs(by) * step
        first = 0 if by >= 0 else narrow - reach
        to = max(by, 0) * step
        update = jnp.dot(
            left[t, :, (2 + by) * octet : (3 + by) * octet],
            ref[t + 2 + by, :, first : first + reach],
            preferred_element_type=jnp.float32,
        )
        if fresh:
            total[t] = update
        else:
            total[t, :, to : to + reach] += update

    def own_terms(ref):
        @pl.loop(0, groups)
        def _(t):
            term(ref, t, 0, True)
            for by in (-2, -1, 1, 2):

                @pl.when(jnp.logical_and(t + by >= 0, t + by < groups))
                def _(by=by):
                    term(ref, t, by)

    def halo_terms(ref, t):
        for by in (-2, -1, 1, 2):
            if not 0 <= t + by < groups:
                term(ref, t, by)

    own_terms(tiles)
    second_halo = halo(square, square_sems)
    waits = {1: (0,), 0: (1,), 2: (2,), 3: (3,)}
    sends = {1: 3, 0: 2, 2: 1, 3: 0}
    for t in (1, 0, 2, 3):
        for n in waits[t]:
            first_halo[n].wait_recv()
        halo_terms(tiles, t)
        for r in range(count):
            at = slice(r * edge, (r + 1) * edge)
            square[t + 2, at, :] = (total[t, at, :] * kept[t, r : r + 1, :]).astype(square.dtype)
        second_halo[{1: 3, 0: 2, 2: 1, 3: 0}[t]].start()

    own_terms(square)
    def delivery(t, n):
        dest, h = n // pair, n % pair
        return remote(
            packed.at[dest, h, t],
            out.at[place.ring, t],
            send.at[n, t],
            recv.at[place.ring, t],
            receivers[n],
        )

    def kept_here(t, n):
        return pltpu.make_async_copy(
            packed.at[n // pair, n % pair, t], out.at[place.ring, t], local.at[t]
        )

    def each_receiver(t, away, here):
        for n, device in enumerate(receivers):

            @pl.when(is_here(device))
            def _(n=n):
                here(kept_here(t, n))

            @pl.when(jnp.logical_not(is_here(device)))
            def _(n=n):
                away(delivery(t, n))

    for t in (1, 0, 2, 3):
        for n in waits[t]:
            second_halo[n].wait_recv()
        halo_terms(square, t)
        for r in range(count):
            at = slice(r * edge, (r + 1) * edge)
            total[t, at, :] = 1.5 * tiles[t + 2, at, :].astype(jnp.float32) - scale * (
                total[t, at, :] * kept[t, r : r + 1, :]
            )
        sorted_rows[...] = jnp.dot(
            sort[...], total[t].astype(packed.dtype), preferred_element_type=jnp.float32
        )
        for n in range(row_devices * halves):
            dest, e = n // halves, n % halves
            at = slice(n * edge, (n + 1) * edge)
            shift = late[n : n + 1, :] > 0.5
            parts = [sorted_rows[at, o * lanes : (o + 1) * lanes] for o in range(narrow // lanes)]
            parts = [jnp.where(shift, two, one) for one, two in zip(parts, parts[1:])]
            turned = [pltpu.roll(part, edge, 1) for part in parts]
            for w in range(len(parts) // 2):
                to = slice(w * lanes, (w + 1) * lanes)
                packed[dest, 0, t, e, :, to] = jnp.where(
                    low, parts[2 * w], turned[2 * w + 1]
                ).astype(packed.dtype)
                packed[dest, 1, t, e, :, to] = jnp.where(
                    low, turned[2 * w], parts[2 * w + 1]
                ).astype(packed.dtype)
        each_receiver(t, lambda copy: copy.start(), lambda copy: copy.start())

    for copy in mark_copies + first_halo + second_halo:
        copy.wait_send()

    @pl.loop(0, 2 * count)
    def _(n):
        copy_of(n, move_sems, target, target_slot, True).wait_send()
        copy_of(n, lane_sems, lane_peer, own_slot).wait_send()
        copy_of(n, core_sems, core_peer, own_slot).wait_send()
        copy_of(n, relay_sems, core_peer, peer_slot).wait_send()

    for t in (1, 0, 2, 3):
        for n, device in enumerate(senders):

            @pl.when(jnp.logical_not(is_here(device)))
            def _(t=t, n=n, device=device):
                remote(
                    packed.at[0, 0, t], out.at[n, t], send.at[0, t], recv.at[n, t], device
                ).wait_recv()

        each_receiver(t, lambda copy: copy.wait_send(), lambda copy: copy.wait())


def band_step(x_vals, occupancy, perm, row_devices, panels, scale):
    count, band, area = x_vals.shape
    edge = BLOCK_EDGE
    lanes = 2 * edge
    octet, wide = count * edge, (band + count) * edge
    narrow = wide // octet * lanes
    halves = panels // row_devices
    supers = perm.shape[0] // (4 * count)
    kind = x_vals.dtype
    rows = (count, edge, band * edge)
    out = (supers, 4, halves, edge, 4 * edge)
    dma = pltpu.SemaphoreType.DMA
    vmem = pl.BlockSpec(memory_space=pltpu.VMEM)
    smem = pl.BlockSpec(memory_space=pltpu.SMEM)
    return pl.pallas_call(
        functools.partial(core_kernel, panels, scale),
        out_shape=jax.ShapeDtypeStruct(out, kind),
        in_specs=[smem, smem, vmem, vmem],
        out_specs=ANY,
        scratch_shapes=[
            pltpu.VMEM(rows, kind),
            pltpu.VMEM((count, wide), kind),
            pltpu.VMEM((octet, lanes), kind),
            pltpu.VMEM((octet, octet), kind),
            pltpu.VMEM((count, lanes), jnp.float32),
            pltpu.VMEM((area // lanes * (band + 8), lanes), jnp.float32),
            pltpu.VMEM((band // 2, edge, lanes), jnp.float32),
            pltpu.VMEM((4,) + rows, kind),
            pltpu.VMEM((4, count, wide), kind),
            pltpu.VMEM((4, octet, wide), kind),
            pltpu.VMEM((8, octet, narrow), kind),
            pltpu.VMEM((8, octet, narrow), kind),
            pltpu.VMEM((4, count, narrow), jnp.float32),
            pltpu.VMEM((4, octet, narrow), jnp.float32),
            pltpu.VMEM((octet, narrow), jnp.float32),
            pltpu.VMEM((row_devices, 2) + out[1:], kind),
            dma((2, 2 * count + 1)),
            dma((2, 2 * count + 1)),
            dma((2, 2 * count + 1)),
            dma((2, 2 * count + 1)),
            dma((2, 4)),
            dma((2, 4)),
            dma((2 * row_devices, 4)),
            dma((supers, 4)),
            dma((4,)),
        ],
        compiler_params=pltpu.CompilerParams(
            collective_id=0, has_side_effects=True, vmem_limit_bytes=60 * 2**20
        ),
        name="band_step",
    )(occupancy, perm, x_vals, occupancy)


def place_kernel(panels, perm, parts_ref, out_ref, origins):
    supers, groups, halves, edge, width = parts_ref.shape
    count = supers * groups
    lanes = 2 * edge
    rows = out_ref.shape[0] // edge
    half = lax.broadcasted_iota(jnp.int32, (edge, lanes), 1) // edge
    first = pl.program_id(0) * rows
    e = first // count

    @pl.when(first == 0)
    def _():
        @pl.loop(0, count)
        def _(n):
            origins[perm[n * panels] % count] = n

    residue = residue_of(perm, panels, count, lax.axis_index("col"))
    spot = residue_of(perm, panels, count, lax.axis_index("row") * halves + e)
    late = (residue < spot).astype(jnp.int32)
    out_ref[...] = jnp.zeros_like(out_ref)

    @pl.loop(0, rows)
    def _(n):
        origin = origins[lax.rem(first + n, count)]
        at = pl.ds(pl.multiple_of(n * edge, edge), edge)
        base = origin - 2 + late + count
        made = []
        for w in range(width // lanes):
            tile = parts_ref[
                origin // groups, lax.rem(origin, groups), e, :, w * lanes : (w + 1) * lanes
            ].astype(jnp.float32)
            rolled = pltpu.roll(tile, edge, 1)
            for side in range(2):
                block = perm[lax.rem(base + 2 * w + side, count) * panels] % count
                odd = lax.rem(block, 2)
                value = jnp.where(odd == side, tile, rolled)
                value = jnp.where(half == odd, value, 0.0).astype(out_ref.dtype)
                made.append((pl.ds(pl.multiple_of((block // 2) * lanes, lanes), lanes), value))
        for to, value in made:
            out_ref[at, to] += value


def place_blocks(parts, perm, panels):
    supers, groups, halves, edge, width = parts.shape
    count = supers * groups
    rows = min(count, 8)
    return pl.pallas_call(
        functools.partial(place_kernel, panels),
        out_shape=jax.ShapeDtypeStruct((halves * count * edge, count * edge), parts.dtype),
        grid_spec=pltpu.PrefetchScalarGridSpec(
            num_scalar_prefetch=1,
            grid=(halves * count // rows,),
            in_specs=[pl.BlockSpec(parts.shape, lambda g, *_: (0, 0, 0, 0, 0))],
            out_specs=pl.BlockSpec((rows * edge, count * edge), lambda g, *_: (g, 0)),
            scratch_shapes=[pltpu.SMEM((count,), jnp.int32)],
        ),
        compiler_params=pltpu.CompilerParams(dimension_semantics=("arbitrary",)),
        name="place_blocks",
    )(perm, parts)


def band_shards(x_vals, occupancy, perm):
    row_devices = lax.axis_size("row")
    panels = lax.axis_size("col")
    band = x_vals.shape[1]
    scale = 0.5 / (BLOCK_EDGE * band)
    parts = band_step(x_vals, occupancy, perm, row_devices, panels, scale)
    return place_blocks(parts, perm, panels)


def shards(x_vals, occupancy, perm):
    row_devices = lax.axis_size("row")
    panels = lax.axis_size("col")
    count, band, _ = x_vals.shape
    if row_devices == 4 and panels == count == 2 * row_devices and band == 4 * count:
        return band_shards(x_vals, occupancy, perm)
    return panel_shards(x_vals, occupancy, perm)


def solution(mesh):
    return jax.shard_map(
        shards,
        mesh=mesh,
        in_specs=(P(("row", "col"), None, None), P(("row", "col"), None), P()),
        out_specs=P("row", "col"),
        check_vma=False,
    )
```

```python
import functools

import jax
import jax.numpy as jnp
from jax import lax
from jax.experimental import pallas as pl
from jax.experimental.pallas import tpu as pltpu
from jax.sharding import PartitionSpec as P

BLOCK_EDGE = 64
MESH = pl.DeviceIdType.MESH
ANY = pl.BlockSpec(memory_space=pl.ANY)


def multiply_kernel(order_ref, left_ref, far0, far1, far2, far3, out_ref):
    width = out_ref.shape[-1]
    left = left_ref[...].reshape(-1, width)
    right = jnp.concatenate([r[...].reshape(-1, width) for r in (far0, far1, far2, far3)], axis=0)
    update = jnp.dot(left, right, preferred_element_type=jnp.float32).reshape(out_ref.shape)

    @pl.when(pl.program_id(1) == 0)
    def _():
        out_ref[...] = update

    @pl.when(pl.program_id(1) != 0)
    def _():
        out_ref[...] += update


def banded_product(left, far, order, residue_major, slots):
    panels, halves, count, edge, width = left.shape
    chunk = slots // 2
    chunks = count // chunk

    def far_spec(position):
        def chunk_of(g):
            return lax.rem(2 * g + chunks - 1 + lax.rem(position + 1 + 2 * g, 4), chunks)

        if residue_major:
            return pl.BlockSpec(
                (1, chunk, edge, width), lambda g, p, order: (order[p], chunk_of(g), 0, 0)
            )
        return pl.BlockSpec(
            (chunk, 1, edge, width), lambda g, p, order: (chunk_of(g), order[p], 0, 0)
        )

    return pl.pallas_call(
        multiply_kernel,
        out_shape=jax.ShapeDtypeStruct((halves, count, edge, width), jnp.float32),
        grid_spec=pltpu.PrefetchScalarGridSpec(
            num_scalar_prefetch=1,
            grid=(count // slots, panels),
            in_specs=[
                pl.BlockSpec(
                    (1, halves, slots, edge, width), lambda g, p, order: (p, 0, g, 0, 0)
                )
            ]
            + [far_spec(position) for position in range(4)],
            out_specs=pl.BlockSpec((halves, slots, edge, width), lambda g, p, order: (0, g, 0, 0)),
        ),
        compiler_params=pltpu.CompilerParams(dimension_semantics=("arbitrary", "arbitrary")),
    )(order, left, far, far, far, far)


def spread_kernel(source_ref, target_ref, rows_ref, out_ref):
    slots = rows_ref.shape[-1] // BLOCK_EDGE
    q, n = pl.program_id(0), pl.program_id(1)
    row = q * pl.num_programs(1) + source_ref[n]
    out_ref[...] = jnp.zeros_like(out_ref)
    for v in range(slots):
        block = rows_ref[0, 0, :, v * BLOCK_EDGE : (v + 1) * BLOCK_EDGE].astype(jnp.float32)
        target = target_ref[row * slots + v]
        odd = lax.rem(target, 2)
        pair = jnp.concatenate(
            [block * (1 - odd).astype(jnp.float32), block * odd.astype(jnp.float32)], axis=1
        ).astype(out_ref.dtype)
        at = pl.multiple_of((target // 2) * (2 * BLOCK_EDGE), 2 * BLOCK_EDGE)
        out_ref[:, pl.ds(at, 2 * BLOCK_EDGE)] += pair


def spread(rows, source, target, panel_cols):
    halves, count, edge, width = rows.shape
    return pl.pallas_call(
        spread_kernel,
        out_shape=jax.ShapeDtypeStruct((halves * count * edge, panel_cols * edge), rows.dtype),
        grid_spec=pltpu.PrefetchScalarGridSpec(
            num_scalar_prefetch=2,
            grid=(halves, count),
            in_specs=[
                pl.BlockSpec((1, 1, edge, width), lambda q, n, source, target: (q, source[n], 0, 0))
            ],
            out_specs=pl.BlockSpec(
                (edge, panel_cols * edge), lambda q, n, source, target: (q * count + n, 0)
            ),
        ),
        compiler_params=pltpu.CompilerParams(dimension_semantics=("arbitrary", "arbitrary")),
    )(source, target, rows)


def band_index(m, row_residue, col_residue, slots):
    first = m - slots // 2 + (col_residue < row_residue).astype(jnp.int32)
    v = jnp.arange(slots, dtype=jnp.int32)
    first = first[..., None]
    return first + (v - first) % slots


def widen(values, index, slots):
    high = (index % (2 * slots)) >= slots
    high = jnp.repeat(high, BLOCK_EDGE, axis=-1)[..., None, :]
    zero = jnp.zeros((), values.dtype)
    return jnp.concatenate(
        [jnp.where(high, zero, values), jnp.where(high, values, zero)], axis=-1
    )


def panel_shards(x_vals, occupancy, perm):
    row_devices = lax.axis_size("row")
    panels = lax.axis_size("col")
    own_row = lax.axis_index("row")
    own_col = lax.axis_index("col")
    local_rows, band_extent, block_area = x_vals.shape
    block_count = perm.shape[0]
    panel_cols = block_count // panels
    halves = panels // row_devices
    slots = band_extent // panels
    lanes = slots * BLOCK_EDGE

    panel_of_residue = perm[:panels] // panel_cols
    residue_ids = jnp.arange(panels, dtype=jnp.int32)
    order = jnp.sum(
        jnp.where(panel_of_residue[None, :] == residue_ids[:, None], residue_ids[None, :], 0), axis=1
    ).astype(jnp.int32)
    inside = perm[::panels] % panel_cols
    m_ids = jnp.arange(panel_cols, dtype=jnp.int32)
    source = jnp.sum(
        jnp.where(inside[None, :] == m_ids[:, None], m_ids[None, :], 0), axis=1
    ).astype(jnp.int32)
    own_residue = order[own_col]
    row_residues = lax.dynamic_slice_in_dim(order, own_row * halves, halves)

    first_row = (own_row * panels + own_col) * local_rows
    row_ids = first_row + jnp.arange(local_rows, dtype=jnp.int32)
    cols = (
        row_ids[:, None] - band_extent // 2 + jnp.arange(band_extent, dtype=jnp.int32)[None, :]
    ) % block_count
    placed = (
        (occupancy[:, :, None, None] == 1)
        & ((cols % panels)[:, :, None, None] == order[None, None, :, None])
        & (
            ((cols // panels) % slots)[:, :, None, None]
            == jnp.arange(slots, dtype=jnp.int32)[None, None, None, :]
        )
    ).astype(jnp.bfloat16)
    kept = jnp.sum(placed.astype(jnp.float32), axis=1).astype(jnp.bfloat16)
    every_kept = lax.all_gather(
        kept.reshape(local_rows, panels * slots), ("row", "col"), axis=0, tiled=True
    ).reshape(panel_cols, panels, panels, slots)
    values = jnp.einsum(
        "kspt,ksf->pktf", placed, x_vals, preferred_element_type=jnp.float32
    ).astype(jnp.bfloat16)
    values = (
        values.reshape(panels, local_rows, slots, BLOCK_EDGE, BLOCK_EDGE)
        .transpose(0, 1, 3, 2, 4)
        .reshape(panels, local_rows, BLOCK_EDGE, lanes)
    )
    first = lax.all_to_all(values, "col", split_axis=0, concat_axis=0, tiled=True)
    first = first.reshape(panels * local_rows, BLOCK_EDGE, lanes)
    far = lax.all_gather(first, "row", axis=0, tiled=True).reshape(
        panel_cols, panels, BLOCK_EDGE, lanes
    )
    tile = jnp.stack(
        [
            lax.dynamic_index_in_dim(far, row_residues[q], axis=1, keepdims=False)
            for q in range(halves)
        ]
    )
    own_kept = lax.dynamic_index_in_dim(every_kept, own_col, axis=2, keepdims=False)
    wanted = jnp.stack(
        [
            lax.dynamic_index_in_dim(own_kept, row_residues[q], axis=1, keepdims=False)
            for q in range(halves)
        ]
    )
    wanted = wanted > 0
    left = lax.all_gather(tile[None], "col", axis=0, tiled=True)

    far_index = band_index(m_ids[:, None], residue_ids[None, :], own_residue, slots)
    far_wide = widen(far, far_index, slots)
    left_index = band_index(
        m_ids[None, None, :], row_residues[None, :, None], order[:, None, None], slots
    )
    left_wide = widen(left, left_index, slots)
    tile_index = band_index(m_ids[None, :], row_residues[:, None], own_residue, slots)
    tile_high = (tile_index % (2 * slots)) >= slots

    def spread_mask(mask):
        return jnp.repeat(mask, BLOCK_EDGE, axis=-1)[:, :, None, :]

    def narrow(wide):
        chosen = jnp.where(spread_mask(tile_high), wide[..., lanes:], wide[..., :lanes])
        return jnp.where(spread_mask(wanted), chosen, 0.0)

    square = narrow(banded_product(left_wide, far_wide, order, False, slots)).astype(jnp.bfloat16)
    far_square = lax.all_gather(square, "row", axis=0, tiled=True)
    square_index = band_index(m_ids[None, :], order[:, None], own_residue, slots)
    square_wide = widen(far_square, square_index, slots)
    cube = narrow(banded_product(left_wide, square_wide, residue_ids, True, slots))
    stepped = (
        1.5 * tile.astype(jnp.float32) - 0.5 / (BLOCK_EDGE * band_extent) * cube
    ).astype(jnp.bfloat16)
    hit = (tile_index % panel_cols)[..., None] == m_ids
    target = jnp.sum(jnp.where(hit, inside, 0), axis=-1).astype(jnp.int32).reshape(-1)
    return spread(stepped, source, target, panel_cols)


class Place:
    def __init__(self, panels):
        self.depth = panels // 2
        self.quarter = panels // 4
        row, col = lax.axis_index("row"), lax.axis_index("col")
        self.half, self.core = row // 2, row % 2
        self.level, self.lane = col // 2, col % 2
        self.step = jnp.where(self.half == 0, self.level, self.depth - 1 - self.level)
        self.ring = self.half * self.depth + self.step

    def device(self, half, core, level, lane):
        return (2 * half + core, 2 * level + lane)

    def at_ring(self, ring):
        half = ring // self.depth
        step = ring % self.depth
        level = jnp.where(half == 0, step, self.depth - 1 - step)
        return self.device(half, self.core, level, self.lane)

    def neighbour(self, by):
        return self.at_ring((self.ring + by + 2 * self.depth) % (2 * self.depth))

    def group_target(self):
        step = self.core * self.quarter + self.level // 2
        level = jnp.where(self.half == 0, step, self.depth - 1 - step)
        return self.device(self.half, 1 - self.level % 2, level, self.lane)

    def group_source(self):
        level = 2 * (self.step % self.quarter) + 1 - self.core
        return self.device(self.half, self.step // self.quarter, level, self.lane)


def remote(source, target, send, recv, device):
    return pltpu.make_async_remote_copy(
        src_ref=source,
        dst_ref=target,
        send_sem=send,
        recv_sem=recv,
        device_id=device,
        device_id_type=MESH,
    )


def residue_of(perm, panels, panel_cols, spot):
    found = jnp.int32(0)
    for n in range(panels):
        found = found + jnp.where(perm[n] // panel_cols == spot, n, 0)
    return found


def core_kernel(
    panels, scale, present, perm, x_vals, flags, out,
    x_ref, rows, marks, pick, sort, late, mid, pairs,
    all_rows, all_marks, left, tiles, square, kept, total, sorted_rows, packed,
    move_sems, lane_sems, core_sems, relay_sems, halo_sems, square_sems, send, recv, local, load_sems,
):
    place = Place(panels)
    row, col = lax.axis_index("row"), lax.axis_index("col")
    count, edge, band_lanes = rows.shape
    octet = count * edge
    groups = all_rows.shape[0]
    wide, narrow = left.shape[-1], tiles.shape[-1]
    width = pick.shape[1]
    row_devices, pair = packed.shape[:2]
    halves = packed.shape[3]
    supers = out.shape[0]

    target, source = place.group_target(), place.group_source()
    lane_peer = place.device(place.half, place.core, place.level, 1 - place.lane)
    core_peer = place.device(place.half, 1 - place.core, place.level, place.lane)
    after, before = place.neighbour(1), place.neighbour(-1)
    target_slot = 2 * (place.level % 2) + place.lane
    own_slot = 2 * (1 - place.core) + place.lane
    peer_slot = 2 * (1 - place.core) + 1 - place.lane
    third_slot = 2 * place.core + place.lane
    last_slot = 2 * place.core + 1 - place.lane
    owner = place.level // 2
    senders = []
    for ring in range(supers):
        half, step = ring // place.depth, ring % place.depth
        level = step if half == 0 else place.depth - 1 - step
        senders.append((2 * half + owner, 2 * level + place.lane))
    receivers = [
        (dest, 2 * (2 * place.core + h) + place.lane)
        for dest in range(row_devices)
        for h in range(pair)
    ]

    def is_here(device):
        return jnp.logical_and(device[0] == row, device[1] == col)

    def load_of(t):
        return pltpu.make_async_copy(x_vals.at[t], x_ref.at[t], load_sems.at[t])

    @pl.loop(0, count)
    def _(t):
        load_of(t).start()

    barrier = pltpu.get_barrier_semaphore()
    for device in (source, lane_peer, core_peer, after, before):
        pl.semaphore_signal(barrier, inc=1, device_id=device, device_id_type=MESH)
    for device in senders:

        @pl.when(jnp.logical_not(is_here(device)))
        def _(device=device):
            pl.semaphore_signal(barrier, inc=1, device_id=device, device_id_type=MESH)

    def piece_of(ref, n):
        return ref.at[n // 2, pl.ds(n % 2 * (edge // 2), edge // 2)]

    def copy_of(n, sems, device, slot, first=False):
        landing = piece_of(all_rows.at[slot], n)
        origin = piece_of(rows, n) if first else landing
        return remote(origin, landing, sems.at[0, n], sems.at[1, n], device)

    def mark_of(sems, device, slot, first=False):
        origin = marks if first else all_marks.at[slot]
        return remote(
            origin, all_marks.at[slot], sems.at[0, 2 * count], sems.at[1, 2 * count], device
        )

    mark_copies = [
        mark_of(move_sems, target, target_slot, True),
        mark_of(lane_sems, lane_peer, own_slot),
        mark_of(core_sems, core_peer, own_slot),
        mark_of(relay_sems, core_peer, peer_slot),
    ]
    lanes = 2 * edge
    low = lax.broadcasted_iota(jnp.int32, (edge, lanes), 1) < edge
    panel_cols = perm.shape[0] // panels
    band, area = x_ref.shape[1:]
    tall = area // lanes
    pitch = mid.shape[0] // tall

    def relay_row(t):
        for p in range(tall):
            mid[p * pitch : p * pitch + band, :] = x_ref[
                t, :, p * lanes : (p + 1) * lanes
            ].astype(jnp.float32)
        for w in range(band // 2):
            one = mid[pl.ds(2 * w, tall, stride=pitch), :] * present[t, 2 * w].astype(jnp.float32)
            two = mid[pl.ds(2 * w + 1, tall, stride=pitch), :] * present[t, 2 * w + 1].astype(
                jnp.float32
            )
            lower = low[:tall]
            pairs[w, pl.ds(0, tall, stride=2), :] = jnp.where(
                lower, one, pltpu.roll(two, edge, 1)
            )
            pairs[w, pl.ds(1, tall, stride=2), :] = jnp.where(
                lower, pltpu.roll(one, edge, 1), two
            )
        for w in range(band // 2):
            rows[t, :, w * lanes : (w + 1) * lanes] = pairs[w].astype(rows.dtype)

    wide_flags = jnp.concatenate([flags[...].astype(jnp.float32)] * count, axis=1)
    at = (count, count * band)
    own = lax.broadcasted_iota(jnp.int32, at, 1) // band == lax.broadcasted_iota(jnp.int32, at, 0)
    to = (count * band, wide)
    entry, lane = (lax.broadcasted_iota(jnp.int32, to, n) for n in range(2))
    spread = (lane // edge - entry // band == entry % band).astype(jnp.float32)
    marks[...] = jnp.dot(
        jnp.where(own, wide_flags, 0.0).astype(marks.dtype),
        spread.astype(marks.dtype),
        preferred_element_type=jnp.float32,
    ).astype(marks.dtype)
    first = 4 * place.core + place.lane
    residues = [residue_of(perm, panels, panel_cols, first + 2 * h) for h in range(2)]
    entry, lane = (lax.broadcasted_iota(jnp.int32, pick.shape, n) for n in range(2))
    base = jnp.where(lane < edge, residues[0] * edge, (residues[1] - 1) * edge)
    pick[...] = (entry == base + lane).astype(jnp.float32).astype(pick.dtype)
    lane = lax.broadcasted_iota(jnp.int32, (1, lanes), 1)
    own = jnp.where(lane < edge, residues[0], residues[1])
    to, entry = (lax.broadcasted_iota(jnp.int32, (edge, octet), n) for n in range(2))
    for n in range(row_devices * halves):
        spot = residue_of(perm, panels, panel_cols, n)
        sort[n * edge : (n + 1) * edge, :] = (
            (entry == to + spot * edge).astype(jnp.float32).astype(sort.dtype)
        )
        late[n : n + 1, :] = (own < spot).astype(jnp.float32)

    expected = 5 + len(receivers)
    pl.semaphore_wait(barrier, jnp.where(owner == place.core, expected - 1, expected))

    mark_copies[0].start()

    @pl.loop(0, count + 1)
    def _(t):
        @pl.when(t < count)
        def _():
            load_of(t).wait()
            relay_row(t)

        @pl.when(t > 0)
        def _():
            for n in range(2):
                copy_of(2 * (t - 1) + n, move_sems, target, target_slot, True).start()

    @pl.loop(0, groups)
    def _(t):
        left[t] = jnp.zeros(left.shape[1:], left.dtype)

    def lay(slot, m):
        base = pl.multiple_of(2 * m * edge, 2 * edge)
        zeros = jnp.zeros((edge, edge), left.dtype)
        reach = pl.ds(base, band_lanes + 2 * edge)
        left[slot, pl.ds(base, edge), pl.ds(base, band_lanes)] = all_rows[slot, 2 * m]
        left[slot, pl.ds(pl.multiple_of(base + edge, edge), edge), reach] = jnp.concatenate(
            [zeros, all_rows[slot, 2 * m + 1], zeros], axis=1
        )
        chosen = pick[...]
        for o in range(wide // octet):
            tiles[slot + 2, pl.ds(base, 2 * edge), o * width : (o + 1) * width] = jnp.dot(
                left[slot, pl.ds(base, 2 * edge), o * octet : (o + 1) * octet],
                chosen,
                preferred_element_type=jnp.float32,
            ).astype(tiles.dtype)

    def halo(ref, sems):
        step = narrow // 5
        moves = (
            (groups + 1, 1, slice(step, narrow), after),
            (groups, 0, slice(2 * step, narrow), after),
            (2, groups + 2, slice(0, 4 * step), before),
            (3, groups + 3, slice(0, 3 * step), before),
        )
        return [
            remote(
                ref.at[origin, :, lanes], ref.at[to, :, lanes], sems.at[0, n], sems.at[1, n], device
            )
            for n, (origin, to, lanes, device) in enumerate(moves)
        ]

    first_halo = halo(tiles, halo_sems)
    sends = {1: 3, 0: 2, 2: 1, 3: 0}

    def send_tile(slot):
        for t in range(groups):

            @pl.when(slot == t)
            def _(t=t):
                first_halo[sends[t]].start()

    rounds = count // 2
    mark_copies[0].wait_recv()
    mark_copies[1].start()
    mark_copies[2].start()

    @pl.loop(0, rounds)
    def _(m):
        for i in range(4):
            n = 4 * m + i
            copy_of(n, move_sems, target, target_slot, True).wait_recv()
            copy_of(n, lane_sems, lane_peer, own_slot).start()
            copy_of(n, core_sems, core_peer, own_slot).start()
        lay(own_slot, m)

    send_tile(own_slot)
    mark_copies[1].wait_recv()
    mark_copies[3].start()

    @pl.loop(0, rounds)
    def _(m):
        for i in range(4):
            n = 4 * m + i
            copy_of(n, lane_sems, lane_peer, own_slot).wait_recv()
            copy_of(n, relay_sems, core_peer, peer_slot).start()
        for i in range(4):
            copy_of(4 * m + i, core_sems, core_peer, own_slot).wait_recv()
        lay(peer_slot, m)
        lay(third_slot, m)

    send_tile(peer_slot)
    send_tile(third_slot)
    @pl.loop(0, rounds)
    def _(m):
        for i in range(4):
            copy_of(4 * m + i, relay_sems, core_peer, peer_slot).wait_recv()
        lay(last_slot, m)

    send_tile(last_slot)

    mark_copies[2].wait_recv()
    mark_copies[3].wait_recv()
    for t in range(groups):
        for o in range(wide // octet):
            kept[t, :, o * width : (o + 1) * width] = jnp.dot(
                all_marks[t, :, o * octet : (o + 1) * octet],
                pick[...],
                preferred_element_type=jnp.float32,
            )

    def term(ref, t, by, fresh=False):
        step = narrow // 5
        reach = narrow - abs(by) * step
        first = 0 if by >= 0 else narrow - reach
        to = max(by, 0) * step
        update = jnp.dot(
            left[t, :, (2 + by) * octet : (3 + by) * octet],
            ref[t + 2 + by, :, first : first + reach],
            preferred_element_type=jnp.float32,
        )
        if fresh:
            total[t] = update
        else:
            total[t, :, to : to + reach] += update

    def own_terms(ref):
        @pl.loop(0, groups)
        def _(t):
            term(ref, t, 0, True)
            for by in (-2, -1, 1, 2):

                @pl.when(jnp.logical_and(t + by >= 0, t + by < groups))
                def _(by=by):
                    term(ref, t, by)

    def halo_terms(ref, t):
        for by in (-2, -1, 1, 2):
            if not 0 <= t + by < groups:
                term(ref, t, by)

    own_terms(tiles)
    second_halo = halo(square, square_sems)
    turns = (1, 2, 0, 3)
    waits = {1: (0,), 0: (1,), 2: (2,), 3: (3,)}
    for t in turns:
        for n in waits[t]:
            first_halo[n].wait_recv()
        halo_terms(tiles, t)
        for r in range(count):
            at = slice(r * edge, (r + 1) * edge)
            square[t + 2, at, :] = (total[t, at, :] * kept[t, r : r + 1, :]).astype(square.dtype)
        second_halo[sends[t]].start()

    own_terms(square)
    def delivery(t, n):
        dest, h = n // pair, n % pair
        return remote(
            packed.at[dest, h, t],
            out.at[place.ring, t],
            send.at[n, t],
            recv.at[place.ring, t],
            receivers[n],
        )

    def kept_here(t, n):
        return pltpu.make_async_copy(
            packed.at[n // pair, n % pair, t], out.at[place.ring, t], local.at[t]
        )

    def each_receiver(t, away, here):
        for n, device in enumerate(receivers):

            @pl.when(is_here(device))
            def _(n=n):
                here(kept_here(t, n))

            @pl.when(jnp.logical_not(is_here(device)))
            def _(n=n):
                away(delivery(t, n))

    for t in turns:
        for n in waits[t]:
            second_halo[n].wait_recv()
        halo_terms(square, t)
        for r in range(count):
            at = slice(r * edge, (r + 1) * edge)
            total[t, at, :] = 1.5 * tiles[t + 2, at, :].astype(jnp.float32) - scale * (
                total[t, at, :] * kept[t, r : r + 1, :]
            )
        sorted_rows[...] = jnp.dot(
            sort[...], total[t].astype(packed.dtype), preferred_element_type=jnp.float32
        )
        for n in range(row_devices * halves):
            dest, e = n // halves, n % halves
            at = slice(n * edge, (n + 1) * edge)
            shift = late[n : n + 1, :] > 0.5
            parts = [sorted_rows[at, o * lanes : (o + 1) * lanes] for o in range(narrow // lanes)]
            parts = [jnp.where(shift, two, one) for one, two in zip(parts, parts[1:])]
            turned = [pltpu.roll(part, edge, 1) for part in parts]
            for w in range(len(parts) // 2):
                to = slice(w * lanes, (w + 1) * lanes)
                packed[dest, 0, t, e, :, to] = jnp.where(
                    low, parts[2 * w], turned[2 * w + 1]
                ).astype(packed.dtype)
                packed[dest, 1, t, e, :, to] = jnp.where(
                    low, turned[2 * w], parts[2 * w + 1]
                ).astype(packed.dtype)
        each_receiver(t, lambda copy: copy.start(), lambda copy: copy.start())

    for copy in mark_copies + first_halo + second_halo:
        copy.wait_send()

    @pl.loop(0, 2 * count)
    def _(n):
        copy_of(n, move_sems, target, target_slot, True).wait_send()
        copy_of(n, lane_sems, lane_peer, own_slot).wait_send()
        copy_of(n, core_sems, core_peer, own_slot).wait_send()
        copy_of(n, relay_sems, core_peer, peer_slot).wait_send()

    for t in turns:
        for n, device in enumerate(senders):

            @pl.when(jnp.logical_not(is_here(device)))
            def _(t=t, n=n, device=device):
                remote(
                    packed.at[0, 0, t], out.at[n, t], send.at[0, t], recv.at[n, t], device
                ).wait_recv()

        each_receiver(t, lambda copy: copy.wait_send(), lambda copy: copy.wait())


def band_step(x_vals, occupancy, perm, row_devices, panels, scale):
    count, band, area = x_vals.shape
    edge = BLOCK_EDGE
    lanes = 2 * edge
    octet, wide = count * edge, (band + count) * edge
    narrow = wide // octet * lanes
    halves = panels // row_devices
    supers = perm.shape[0] // (4 * count)
    kind = x_vals.dtype
    rows = (count, edge, band * edge)
    out = (supers, 4, halves, edge, 4 * edge)
    dma = pltpu.SemaphoreType.DMA
    vmem = pl.BlockSpec(memory_space=pltpu.VMEM)
    smem = pl.BlockSpec(memory_space=pltpu.SMEM)
    return pl.pallas_call(
        functools.partial(core_kernel, panels, scale),
        out_shape=jax.ShapeDtypeStruct(out, kind),
        in_specs=[smem, smem, ANY, vmem],
        out_specs=ANY,
        scratch_shapes=[
            pltpu.VMEM(x_vals.shape, kind),
            pltpu.VMEM(rows, kind),
            pltpu.VMEM((count, wide), kind),
            pltpu.VMEM((octet, lanes), kind),
            pltpu.VMEM((octet, octet), kind),
            pltpu.VMEM((count, lanes), jnp.float32),
            pltpu.VMEM((area // lanes * (band + 8), lanes), jnp.float32),
            pltpu.VMEM((band // 2, edge, lanes), jnp.float32),
            pltpu.VMEM((4,) + rows, kind),
            pltpu.VMEM((4, count, wide), kind),
            pltpu.VMEM((4, octet, wide), kind),
            pltpu.VMEM((8, octet, narrow), kind),
            pltpu.VMEM((8, octet, narrow), kind),
            pltpu.VMEM((4, count, narrow), jnp.float32),
            pltpu.VMEM((4, octet, narrow), jnp.float32),
            pltpu.VMEM((octet, narrow), jnp.float32),
            pltpu.VMEM((row_devices, 2) + out[1:], kind),
            dma((2, 2 * count + 1)),
            dma((2, 2 * count + 1)),
            dma((2, 2 * count + 1)),
            dma((2, 2 * count + 1)),
            dma((2, 4)),
            dma((2, 4)),
            dma((2 * row_devices, 4)),
            dma((supers, 4)),
            dma((4,)),
            dma((count,)),
        ],
        compiler_params=pltpu.CompilerParams(
            collective_id=0, has_side_effects=True, vmem_limit_bytes=60 * 2**20
        ),
        name="band_step",
    )(occupancy, perm, x_vals, occupancy)


def place_kernel(panels, perm, parts_ref, out_ref, origins):
    supers, groups, halves, edge, width = parts_ref.shape
    count = supers * groups
    lanes = 2 * edge
    rows = out_ref.shape[0] // edge
    half = lax.broadcasted_iota(jnp.int32, (edge, lanes), 1) // edge
    first = pl.program_id(0) * rows
    e = first // count

    @pl.when(first == 0)
    def _():
        @pl.loop(0, count)
        def _(n):
            origins[perm[n * panels] % count] = n

    residue = residue_of(perm, panels, count, lax.axis_index("col"))
    spot = residue_of(perm, panels, count, lax.axis_index("row") * halves + e)
    late = (residue < spot).astype(jnp.int32)
    out_ref[...] = jnp.zeros_like(out_ref)

    for n in range(rows):
        origin = origins[lax.rem(first + n, count)]
        at = slice(n * edge, (n + 1) * edge)
        base = origin - 2 + late + count
        made = []
        for w in range(width // lanes):
            tile = parts_ref[
                origin // groups, lax.rem(origin, groups), e, :, w * lanes : (w + 1) * lanes
            ].astype(jnp.float32)
            rolled = pltpu.roll(tile, edge, 1)
            for side in range(2):
                block = perm[lax.rem(base + 2 * w + side, count) * panels] % count
                odd = lax.rem(block, 2)
                value = jnp.where(odd == side, tile, rolled)
                value = jnp.where(half == odd, value, 0.0).astype(out_ref.dtype)
                made.append((pl.ds(pl.multiple_of((block // 2) * lanes, lanes), lanes), value))
        for to, value in made:
            out_ref[at, to] += value


def place_blocks(parts, perm, panels):
    supers, groups, halves, edge, width = parts.shape
    count = supers * groups
    rows = min(count, 8)
    return pl.pallas_call(
        functools.partial(place_kernel, panels),
        out_shape=jax.ShapeDtypeStruct((halves * count * edge, count * edge), parts.dtype),
        grid_spec=pltpu.PrefetchScalarGridSpec(
            num_scalar_prefetch=1,
            grid=(halves * count // rows,),
            in_specs=[pl.BlockSpec(parts.shape, lambda g, *_: (0, 0, 0, 0, 0))],
            out_specs=pl.BlockSpec((rows * edge, count * edge), lambda g, *_: (g, 0)),
            scratch_shapes=[pltpu.SMEM((count,), jnp.int32)],
        ),
        compiler_params=pltpu.CompilerParams(dimension_semantics=("arbitrary",)),
        name="place_blocks",
    )(perm, parts)


def band_shards(x_vals, occupancy, perm):
    row_devices = lax.axis_size("row")
    panels = lax.axis_size("col")
    band = x_vals.shape[1]
    scale = 0.5 / (BLOCK_EDGE * band)
    parts = band_step(x_vals, occupancy, perm, row_devices, panels, scale)
    return place_blocks(parts, perm, panels)


def shards(x_vals, occupancy, perm):
    row_devices = lax.axis_size("row")
    panels = lax.axis_size("col")
    count, band, _ = x_vals.shape
    if row_devices == 4 and panels == count == 2 * row_devices and band == 4 * count:
        return band_shards(x_vals, occupancy, perm)
    return panel_shards(x_vals, occupancy, perm)


def solution(mesh):
    return jax.shard_map(
        shards,
        mesh=mesh,
        in_specs=(P(("row", "col"), None, None), P(("row", "col"), None), P()),
        out_specs=P("row", "col"),
        check_vma=False,
    )
```

```python
import functools

import jax
import jax.numpy as jnp
from jax import lax
from jax.experimental import pallas as pl
from jax.experimental.pallas import tpu as pltpu
from jax.sharding import PartitionSpec as P

BLOCK_EDGE = 64
MESH = pl.DeviceIdType.MESH
ANY = pl.BlockSpec(memory_space=pl.ANY)


def multiply_kernel(order_ref, left_ref, far0, far1, far2, far3, out_ref):
    width = out_ref.shape[-1]
    left = left_ref[...].reshape(-1, width)
    right = jnp.concatenate([r[...].reshape(-1, width) for r in (far0, far1, far2, far3)], axis=0)
    update = jnp.dot(left, right, preferred_element_type=jnp.float32).reshape(out_ref.shape)

    @pl.when(pl.program_id(1) == 0)
    def _():
        out_ref[...] = update

    @pl.when(pl.program_id(1) != 0)
    def _():
        out_ref[...] += update


def banded_product(left, far, order, residue_major, slots):
    panels, halves, count, edge, width = left.shape
    chunk = slots // 2
    chunks = count // chunk

    def far_spec(position):
        def chunk_of(g):
            return lax.rem(2 * g + chunks - 1 + lax.rem(position + 1 + 2 * g, 4), chunks)

        if residue_major:
            return pl.BlockSpec(
                (1, chunk, edge, width), lambda g, p, order: (order[p], chunk_of(g), 0, 0)
            )
        return pl.BlockSpec(
            (chunk, 1, edge, width), lambda g, p, order: (chunk_of(g), order[p], 0, 0)
        )

    return pl.pallas_call(
        multiply_kernel,
        out_shape=jax.ShapeDtypeStruct((halves, count, edge, width), jnp.float32),
        grid_spec=pltpu.PrefetchScalarGridSpec(
            num_scalar_prefetch=1,
            grid=(count // slots, panels),
            in_specs=[
                pl.BlockSpec(
                    (1, halves, slots, edge, width), lambda g, p, order: (p, 0, g, 0, 0)
                )
            ]
            + [far_spec(position) for position in range(4)],
            out_specs=pl.BlockSpec((halves, slots, edge, width), lambda g, p, order: (0, g, 0, 0)),
        ),
        compiler_params=pltpu.CompilerParams(dimension_semantics=("arbitrary", "arbitrary")),
    )(order, left, far, far, far, far)


def spread_kernel(source_ref, target_ref, rows_ref, out_ref):
    slots = rows_ref.shape[-1] // BLOCK_EDGE
    q, n = pl.program_id(0), pl.program_id(1)
    row = q * pl.num_programs(1) + source_ref[n]
    out_ref[...] = jnp.zeros_like(out_ref)
    for v in range(slots):
        block = rows_ref[0, 0, :, v * BLOCK_EDGE : (v + 1) * BLOCK_EDGE].astype(jnp.float32)
        target = target_ref[row * slots + v]
        odd = lax.rem(target, 2)
        pair = jnp.concatenate(
            [block * (1 - odd).astype(jnp.float32), block * odd.astype(jnp.float32)], axis=1
        ).astype(out_ref.dtype)
        at = pl.multiple_of((target // 2) * (2 * BLOCK_EDGE), 2 * BLOCK_EDGE)
        out_ref[:, pl.ds(at, 2 * BLOCK_EDGE)] += pair


def spread(rows, source, target, panel_cols):
    halves, count, edge, width = rows.shape
    return pl.pallas_call(
        spread_kernel,
        out_shape=jax.ShapeDtypeStruct((halves * count * edge, panel_cols * edge), rows.dtype),
        grid_spec=pltpu.PrefetchScalarGridSpec(
            num_scalar_prefetch=2,
            grid=(halves, count),
            in_specs=[
                pl.BlockSpec((1, 1, edge, width), lambda q, n, source, target: (q, source[n], 0, 0))
            ],
            out_specs=pl.BlockSpec(
                (edge, panel_cols * edge), lambda q, n, source, target: (q * count + n, 0)
            ),
        ),
        compiler_params=pltpu.CompilerParams(dimension_semantics=("arbitrary", "arbitrary")),
    )(source, target, rows)


def band_index(m, row_residue, col_residue, slots):
    first = m - slots // 2 + (col_residue < row_residue).astype(jnp.int32)
    v = jnp.arange(slots, dtype=jnp.int32)
    first = first[..., None]
    return first + (v - first) % slots


def widen(values, index, slots):
    high = (index % (2 * slots)) >= slots
    high = jnp.repeat(high, BLOCK_EDGE, axis=-1)[..., None, :]
    zero = jnp.zeros((), values.dtype)
    return jnp.concatenate(
        [jnp.where(high, zero, values), jnp.where(high, values, zero)], axis=-1
    )


def panel_shards(x_vals, occupancy, perm):
    row_devices = lax.axis_size("row")
    panels = lax.axis_size("col")
    own_row = lax.axis_index("row")
    own_col = lax.axis_index("col")
    local_rows, band_extent, block_area = x_vals.shape
    block_count = perm.shape[0]
    panel_cols = block_count // panels
    halves = panels // row_devices
    slots = band_extent // panels
    lanes = slots * BLOCK_EDGE

    panel_of_residue = perm[:panels] // panel_cols
    residue_ids = jnp.arange(panels, dtype=jnp.int32)
    order = jnp.sum(
        jnp.where(panel_of_residue[None, :] == residue_ids[:, None], residue_ids[None, :], 0), axis=1
    ).astype(jnp.int32)
    inside = perm[::panels] % panel_cols
    m_ids = jnp.arange(panel_cols, dtype=jnp.int32)
    source = jnp.sum(
        jnp.where(inside[None, :] == m_ids[:, None], m_ids[None, :], 0), axis=1
    ).astype(jnp.int32)
    own_residue = order[own_col]
    row_residues = lax.dynamic_slice_in_dim(order, own_row * halves, halves)

    first_row = (own_row * panels + own_col) * local_rows
    row_ids = first_row + jnp.arange(local_rows, dtype=jnp.int32)
    cols = (
        row_ids[:, None] - band_extent // 2 + jnp.arange(band_extent, dtype=jnp.int32)[None, :]
    ) % block_count
    placed = (
        (occupancy[:, :, None, None] == 1)
        & ((cols % panels)[:, :, None, None] == order[None, None, :, None])
        & (
            ((cols // panels) % slots)[:, :, None, None]
            == jnp.arange(slots, dtype=jnp.int32)[None, None, None, :]
        )
    ).astype(jnp.bfloat16)
    kept = jnp.sum(placed.astype(jnp.float32), axis=1).astype(jnp.bfloat16)
    every_kept = lax.all_gather(
        kept.reshape(local_rows, panels * slots), ("row", "col"), axis=0, tiled=True
    ).reshape(panel_cols, panels, panels, slots)
    values = jnp.einsum(
        "kspt,ksf->pktf", placed, x_vals, preferred_element_type=jnp.float32
    ).astype(jnp.bfloat16)
    values = (
        values.reshape(panels, local_rows, slots, BLOCK_EDGE, BLOCK_EDGE)
        .transpose(0, 1, 3, 2, 4)
        .reshape(panels, local_rows, BLOCK_EDGE, lanes)
    )
    first = lax.all_to_all(values, "col", split_axis=0, concat_axis=0, tiled=True)
    first = first.reshape(panels * local_rows, BLOCK_EDGE, lanes)
    far = lax.all_gather(first, "row", axis=0, tiled=True).reshape(
        panel_cols, panels, BLOCK_EDGE, lanes
    )
    tile = jnp.stack(
        [
            lax.dynamic_index_in_dim(far, row_residues[q], axis=1, keepdims=False)
            for q in range(halves)
        ]
    )
    own_kept = lax.dynamic_index_in_dim(every_kept, own_col, axis=2, keepdims=False)
    wanted = jnp.stack(
        [
            lax.dynamic_index_in_dim(own_kept, row_residues[q], axis=1, keepdims=False)
            for q in range(halves)
        ]
    )
    wanted = wanted > 0
    left = lax.all_gather(tile[None], "col", axis=0, tiled=True)

    far_index = band_index(m_ids[:, None], residue_ids[None, :], own_residue, slots)
    far_wide = widen(far, far_index, slots)
    left_index = band_index(
        m_ids[None, None, :], row_residues[None, :, None], order[:, None, None], slots
    )
    left_wide = widen(left, left_index, slots)
    tile_index = band_index(m_ids[None, :], row_residues[:, None], own_residue, slots)
    tile_high = (tile_index % (2 * slots)) >= slots

    def spread_mask(mask):
        return jnp.repeat(mask, BLOCK_EDGE, axis=-1)[:, :, None, :]

    def narrow(wide):
        chosen = jnp.where(spread_mask(tile_high), wide[..., lanes:], wide[..., :lanes])
        return jnp.where(spread_mask(wanted), chosen, 0.0)

    square = narrow(banded_product(left_wide, far_wide, order, False, slots)).astype(jnp.bfloat16)
    far_square = lax.all_gather(square, "row", axis=0, tiled=True)
    square_index = band_index(m_ids[None, :], order[:, None], own_residue, slots)
    square_wide = widen(far_square, square_index, slots)
    cube = narrow(banded_product(left_wide, square_wide, residue_ids, True, slots))
    stepped = (
        1.5 * tile.astype(jnp.float32) - 0.5 / (BLOCK_EDGE * band_extent) * cube
    ).astype(jnp.bfloat16)
    hit = (tile_index % panel_cols)[..., None] == m_ids
    target = jnp.sum(jnp.where(hit, inside, 0), axis=-1).astype(jnp.int32).reshape(-1)
    return spread(stepped, source, target, panel_cols)


class Place:
    def __init__(self, panels):
        self.depth = panels // 2
        self.quarter = panels // 4
        row, col = lax.axis_index("row"), lax.axis_index("col")
        self.half, self.core = row // 2, row % 2
        self.level, self.lane = col // 2, col % 2
        self.step = jnp.where(self.half == 0, self.level, self.depth - 1 - self.level)
        self.ring = self.half * self.depth + self.step

    def device(self, half, core, level, lane):
        return (2 * half + core, 2 * level + lane)

    def at_ring(self, ring):
        half = ring // self.depth
        step = ring % self.depth
        level = jnp.where(half == 0, step, self.depth - 1 - step)
        return self.device(half, self.core, level, self.lane)

    def neighbour(self, by):
        return self.at_ring((self.ring + by + 2 * self.depth) % (2 * self.depth))

    def group_target(self):
        step = self.core * self.quarter + self.level // 2
        level = jnp.where(self.half == 0, step, self.depth - 1 - step)
        return self.device(self.half, 1 - self.level % 2, level, self.lane)

    def group_source(self):
        level = 2 * (self.step % self.quarter) + 1 - self.core
        return self.device(self.half, self.step // self.quarter, level, self.lane)


def remote(source, target, send, recv, device):
    return pltpu.make_async_remote_copy(
        src_ref=source,
        dst_ref=target,
        send_sem=send,
        recv_sem=recv,
        device_id=device,
        device_id_type=MESH,
    )


def residue_of(perm, panels, panel_cols, spot):
    found = jnp.int32(0)
    for n in range(panels):
        found = found + jnp.where(perm[n] // panel_cols == spot, n, 0)
    return found


def core_kernel(
    panels, scale, present, perm, x_vals, flags, out,
    x_ref, rows, marks, pick, sort, late, mid, pairs,
    all_rows, all_marks, left, tiles, square, kept, total, sorted_rows, packed,
    move_sems, lane_sems, core_sems, relay_sems, halo_sems, square_sems, send, recv, local, load_sems,
):
    place = Place(panels)
    row, col = lax.axis_index("row"), lax.axis_index("col")
    count, edge, band_lanes = rows.shape
    octet = count * edge
    groups = all_rows.shape[0]
    wide, narrow = left.shape[-1], tiles.shape[-1]
    width = pick.shape[1]
    row_devices, pair = packed.shape[:2]
    halves = packed.shape[3]
    supers = out.shape[0]

    target, source = place.group_target(), place.group_source()
    lane_peer = place.device(place.half, place.core, place.level, 1 - place.lane)
    core_peer = place.device(place.half, 1 - place.core, place.level, place.lane)
    after, before = place.neighbour(1), place.neighbour(-1)
    target_slot = 2 * (place.level % 2) + place.lane
    own_slot = 2 * (1 - place.core) + place.lane
    peer_slot = 2 * (1 - place.core) + 1 - place.lane
    third_slot = 2 * place.core + place.lane
    last_slot = 2 * place.core + 1 - place.lane
    owner = place.level // 2
    senders = []
    for ring in range(supers):
        half, step = ring // place.depth, ring % place.depth
        level = step if half == 0 else place.depth - 1 - step
        senders.append((2 * half + owner, 2 * level + place.lane))
    receivers = [
        (dest, 2 * (2 * place.core + h) + place.lane)
        for dest in range(row_devices)
        for h in range(pair)
    ]

    def is_here(device):
        return jnp.logical_and(device[0] == row, device[1] == col)

    def load_of(t):
        return pltpu.make_async_copy(x_vals.at[t], x_ref.at[t], load_sems.at[t])

    @pl.loop(0, count)
    def _(t):
        load_of(t).start()

    barrier = pltpu.get_barrier_semaphore()
    for device in (source, lane_peer, core_peer, after, before):
        pl.semaphore_signal(barrier, inc=1, device_id=device, device_id_type=MESH)
    for device in senders:

        @pl.when(jnp.logical_not(is_here(device)))
        def _(device=device):
            pl.semaphore_signal(barrier, inc=1, device_id=device, device_id_type=MESH)

    def piece_of(ref, n):
        return ref.at[n // 2, pl.ds(n % 2 * (edge // 2), edge // 2)]

    def copy_of(n, sems, device, slot, first=False):
        landing = piece_of(all_rows.at[slot], n)
        origin = piece_of(rows, n) if first else landing
        return remote(origin, landing, sems.at[0, n], sems.at[1, n], device)

    def mark_of(sems, device, slot, first=False):
        origin = marks if first else all_marks.at[slot]
        return remote(
            origin, all_marks.at[slot], sems.at[0, 2 * count], sems.at[1, 2 * count], device
        )

    mark_copies = [
        mark_of(move_sems, target, target_slot, True),
        mark_of(lane_sems, lane_peer, own_slot),
        mark_of(core_sems, core_peer, own_slot),
        mark_of(relay_sems, core_peer, peer_slot),
    ]
    lanes = 2 * edge
    low = lax.broadcasted_iota(jnp.int32, (edge, lanes), 1) < edge
    panel_cols = perm.shape[0] // panels
    band, area = x_ref.shape[1:]
    tall = area // lanes
    pitch = mid.shape[0] // tall

    def relay_row(t):
        for p in range(tall):
            mid[p * pitch : p * pitch + band, :] = x_ref[
                t, :, p * lanes : (p + 1) * lanes
            ].astype(jnp.float32)
        for w in range(band // 2):
            one = mid[pl.ds(2 * w, tall, stride=pitch), :] * present[t, 2 * w].astype(jnp.float32)
            two = mid[pl.ds(2 * w + 1, tall, stride=pitch), :] * present[t, 2 * w + 1].astype(
                jnp.float32
            )
            lower = low[:tall]
            pairs[w, pl.ds(0, tall, stride=2), :] = jnp.where(
                lower, one, pltpu.roll(two, edge, 1)
            )
            pairs[w, pl.ds(1, tall, stride=2), :] = jnp.where(
                lower, pltpu.roll(one, edge, 1), two
            )
        for w in range(band // 2):
            rows[t, :, w * lanes : (w + 1) * lanes] = pairs[w].astype(rows.dtype)

    wide_flags = jnp.concatenate([flags[...].astype(jnp.float32)] * count, axis=1)
    at = (count, count * band)
    own = lax.broadcasted_iota(jnp.int32, at, 1) // band == lax.broadcasted_iota(jnp.int32, at, 0)
    to = (count * band, wide)
    entry, lane = (lax.broadcasted_iota(jnp.int32, to, n) for n in range(2))
    spread = (lane // edge - entry // band == entry % band).astype(jnp.float32)
    marks[...] = jnp.dot(
        jnp.where(own, wide_flags, 0.0).astype(marks.dtype),
        spread.astype(marks.dtype),
        preferred_element_type=jnp.float32,
    ).astype(marks.dtype)
    first = 4 * place.core + place.lane
    residues = [residue_of(perm, panels, panel_cols, first + 2 * h) for h in range(2)]
    entry, lane = (lax.broadcasted_iota(jnp.int32, pick.shape, n) for n in range(2))
    base = jnp.where(lane < edge, residues[0] * edge, (residues[1] - 1) * edge)
    pick[...] = (entry == base + lane).astype(jnp.float32).astype(pick.dtype)
    lane = lax.broadcasted_iota(jnp.int32, (1, lanes), 1)
    own = jnp.where(lane < edge, residues[0], residues[1])
    to, entry = (lax.broadcasted_iota(jnp.int32, (edge, octet), n) for n in range(2))
    for n in range(row_devices * halves):
        spot = residue_of(perm, panels, panel_cols, n)
        sort[n * edge : (n + 1) * edge, :] = (
            (entry == to + spot * edge).astype(jnp.float32).astype(sort.dtype)
        )
        late[n : n + 1, :] = (own < spot).astype(jnp.float32)

    expected = 5 + len(receivers)
    pl.semaphore_wait(barrier, jnp.where(owner == place.core, expected - 1, expected))

    mark_copies[0].start()

    @pl.loop(0, count + 1)
    def _(t):
        @pl.when(t < count)
        def _():
            load_of(t).wait()
            relay_row(t)

        @pl.when(t > 0)
        def _():
            for n in range(2):
                copy_of(2 * (t - 1) + n, move_sems, target, target_slot, True).start()

    @pl.loop(0, groups)
    def _(t):
        left[t] = jnp.zeros(left.shape[1:], left.dtype)

    def lay(slot, m):
        base = pl.multiple_of(2 * m * edge, 2 * edge)
        zeros = jnp.zeros((edge, edge), left.dtype)
        reach = pl.ds(base, band_lanes + 2 * edge)
        left[slot, pl.ds(base, edge), pl.ds(base, band_lanes)] = all_rows[slot, 2 * m]
        left[slot, pl.ds(pl.multiple_of(base + edge, edge), edge), reach] = jnp.concatenate(
            [zeros, all_rows[slot, 2 * m + 1], zeros], axis=1
        )
        chosen = pick[...]
        for o in range(wide // octet):
            tiles[slot + 2, pl.ds(base, 2 * edge), o * width : (o + 1) * width] = jnp.dot(
                left[slot, pl.ds(base, 2 * edge), o * octet : (o + 1) * octet],
                chosen,
                preferred_element_type=jnp.float32,
            ).astype(tiles.dtype)

    def halo(ref, sems):
        step = narrow // 5
        moves = (
            (groups + 1, 1, slice(step, narrow), after),
            (groups, 0, slice(2 * step, narrow), after),
            (2, groups + 2, slice(0, 4 * step), before),
            (3, groups + 3, slice(0, 3 * step), before),
        )
        return [
            remote(
                ref.at[origin, :, lanes], ref.at[to, :, lanes], sems.at[0, n], sems.at[1, n], device
            )
            for n, (origin, to, lanes, device) in enumerate(moves)
        ]

    first_halo = halo(tiles, halo_sems)
    sends = {1: 3, 0: 2, 2: 1, 3: 0}

    def send_tile(slot):
        for t in range(groups):

            @pl.when(slot == t)
            def _(t=t):
                first_halo[sends[t]].start()

    rounds = count // 2
    mark_copies[0].wait_recv()
    mark_copies[1].start()
    mark_copies[2].start()

    @pl.loop(0, rounds)
    def _(m):
        for i in range(4):
            n = 4 * m + i
            copy_of(n, move_sems, target, target_slot, True).wait_recv()
            copy_of(n, lane_sems, lane_peer, own_slot).start()
            copy_of(n, core_sems, core_peer, own_slot).start()
        lay(own_slot, m)

    send_tile(own_slot)
    mark_copies[1].wait_recv()
    mark_copies[3].start()

    @pl.loop(0, rounds)
    def _(m):
        for i in range(4):
            n = 4 * m + i
            copy_of(n, lane_sems, lane_peer, own_slot).wait_recv()
            copy_of(n, relay_sems, core_peer, peer_slot).start()
        for i in range(4):
            copy_of(4 * m + i, core_sems, core_peer, own_slot).wait_recv()
        lay(peer_slot, m)
        lay(third_slot, m)

    send_tile(peer_slot)
    send_tile(third_slot)
    @pl.loop(0, rounds)
    def _(m):
        for i in range(4):
            copy_of(4 * m + i, relay_sems, core_peer, peer_slot).wait_recv()
        lay(last_slot, m)

    send_tile(last_slot)

    mark_copies[2].wait_recv()
    mark_copies[3].wait_recv()
    for t in range(groups):
        for o in range(wide // octet):
            kept[t, :, o * width : (o + 1) * width] = jnp.dot(
                all_marks[t, :, o * octet : (o + 1) * octet],
                pick[...],
                preferred_element_type=jnp.float32,
            )

    def term(ref, t, by, fresh=False):
        step = narrow // 5
        reach = narrow - abs(by) * step
        first = 0 if by >= 0 else narrow - reach
        to = max(by, 0) * step
        update = jnp.dot(
            left[t, :, (2 + by) * octet : (3 + by) * octet],
            ref[t + 2 + by, :, first : first + reach],
            preferred_element_type=jnp.float32,
        )
        if fresh:
            total[t] = update
        else:
            total[t, :, to : to + reach] += update

    def own_terms(ref):
        @pl.loop(0, groups)
        def _(t):
            term(ref, t, 0, True)
            for by in (-2, -1, 1, 2):

                @pl.when(jnp.logical_and(t + by >= 0, t + by < groups))
                def _(by=by):
                    term(ref, t, by)

    def halo_terms(ref, t):
        for by in (-2, -1, 1, 2):
            if not 0 <= t + by < groups:
                term(ref, t, by)

    own_terms(tiles)
    second_halo = halo(square, square_sems)
    turns = (0, 3, 1, 2)
    reads = {0: (0, 1), 1: (0,), 2: (2,), 3: (2, 3)}
    waited = set()
    for t in turns:
        for n in reads[t]:
            if n not in waited:
                first_halo[n].wait_recv()
                waited.add(n)
        halo_terms(tiles, t)
        for r in range(count):
            at = slice(r * edge, (r + 1) * edge)
            square[t + 2, at, :] = (total[t, at, :] * kept[t, r : r + 1, :]).astype(square.dtype)
        second_halo[sends[t]].start()

    own_terms(square)
    turns = (1, 2, 0, 3)
    def delivery(t, n):
        dest, h = n // pair, n % pair
        return remote(
            packed.at[dest, h, t],
            out.at[place.ring, t],
            send.at[n, t],
            recv.at[place.ring, t],
            receivers[n],
        )

    def kept_here(t, n):
        return pltpu.make_async_copy(
            packed.at[n // pair, n % pair, t], out.at[place.ring, t], local.at[t]
        )

    def each_receiver(t, away, here):
        for n, device in enumerate(receivers):

            @pl.when(is_here(device))
            def _(n=n):
                here(kept_here(t, n))

            @pl.when(jnp.logical_not(is_here(device)))
            def _(n=n):
                away(delivery(t, n))

    waited = set()
    for t in turns:
        for n in reads[t]:
            if n not in waited:
                second_halo[n].wait_recv()
                waited.add(n)
        halo_terms(square, t)
        for r in range(count):
            at = slice(r * edge, (r + 1) * edge)
            total[t, at, :] = 1.5 * tiles[t + 2, at, :].astype(jnp.float32) - scale * (
                total[t, at, :] * kept[t, r : r + 1, :]
            )
        sorted_rows[...] = jnp.dot(
            sort[...], total[t].astype(packed.dtype), preferred_element_type=jnp.float32
        )
        for n in range(row_devices * halves):
            dest, e = n // halves, n % halves
            at = slice(n * edge, (n + 1) * edge)
            shift = late[n : n + 1, :] > 0.5
            parts = [sorted_rows[at, o * lanes : (o + 1) * lanes] for o in range(narrow // lanes)]
            parts = [jnp.where(shift, two, one) for one, two in zip(parts, parts[1:])]
            turned = [pltpu.roll(part, edge, 1) for part in parts]
            for w in range(len(parts) // 2):
                to = slice(w * lanes, (w + 1) * lanes)
                packed[dest, 0, t, e, :, to] = jnp.where(
                    low, parts[2 * w], turned[2 * w + 1]
                ).astype(packed.dtype)
                packed[dest, 1, t, e, :, to] = jnp.where(
                    low, turned[2 * w], parts[2 * w + 1]
                ).astype(packed.dtype)
        each_receiver(t, lambda copy: copy.start(), lambda copy: copy.start())

    for copy in mark_copies + first_halo + second_halo:
        copy.wait_send()

    @pl.loop(0, 2 * count)
    def _(n):
        copy_of(n, move_sems, target, target_slot, True).wait_send()
        copy_of(n, lane_sems, lane_peer, own_slot).wait_send()
        copy_of(n, core_sems, core_peer, own_slot).wait_send()
        copy_of(n, relay_sems, core_peer, peer_slot).wait_send()

    for t in turns:
        for n, device in enumerate(senders):

            @pl.when(jnp.logical_not(is_here(device)))
            def _(t=t, n=n, device=device):
                remote(
                    packed.at[0, 0, t], out.at[n, t], send.at[0, t], recv.at[n, t], device
                ).wait_recv()

        each_receiver(t, lambda copy: copy.wait_send(), lambda copy: copy.wait())


def band_step(x_vals, occupancy, perm, row_devices, panels, scale):
    count, band, area = x_vals.shape
    edge = BLOCK_EDGE
    lanes = 2 * edge
    octet, wide = count * edge, (band + count) * edge
    narrow = wide // octet * lanes
    halves = panels // row_devices
    supers = perm.shape[0] // (4 * count)
    kind = x_vals.dtype
    rows = (count, edge, band * edge)
    out = (supers, 4, halves, edge, 4 * edge)
    dma = pltpu.SemaphoreType.DMA
    vmem = pl.BlockSpec(memory_space=pltpu.VMEM)
    smem = pl.BlockSpec(memory_space=pltpu.SMEM)
    return pl.pallas_call(
        functools.partial(core_kernel, panels, scale),
        out_shape=jax.ShapeDtypeStruct(out, kind),
        in_specs=[smem, smem, ANY, vmem],
        out_specs=ANY,
        scratch_shapes=[
            pltpu.VMEM(x_vals.shape, kind),
            pltpu.VMEM(rows, kind),
            pltpu.VMEM((count, wide), kind),
            pltpu.VMEM((octet, lanes), kind),
            pltpu.VMEM((octet, octet), kind),
            pltpu.VMEM((count, lanes), jnp.float32),
            pltpu.VMEM((area // lanes * (band + 8), lanes), jnp.float32),
            pltpu.VMEM((band // 2, edge, lanes), jnp.float32),
            pltpu.VMEM((4,) + rows, kind),
            pltpu.VMEM((4, count, wide), kind),
            pltpu.VMEM((4, octet, wide), kind),
            pltpu.VMEM((8, octet, narrow), kind),
            pltpu.VMEM((8, octet, narrow), kind),
            pltpu.VMEM((4, count, narrow), jnp.float32),
            pltpu.VMEM((4, octet, narrow), jnp.float32),
            pltpu.VMEM((octet, narrow), jnp.float32),
            pltpu.VMEM((row_devices, 2) + out[1:], kind),
            dma((2, 2 * count + 1)),
            dma((2, 2 * count + 1)),
            dma((2, 2 * count + 1)),
            dma((2, 2 * count + 1)),
            dma((2, 4)),
            dma((2, 4)),
            dma((2 * row_devices, 4)),
            dma((supers, 4)),
            dma((4,)),
            dma((count,)),
        ],
        compiler_params=pltpu.CompilerParams(
            collective_id=0, has_side_effects=True, vmem_limit_bytes=60 * 2**20
        ),
        name="band_step",
    )(occupancy, perm, x_vals, occupancy)


def place_kernel(panels, perm, parts_in, out, parts, canvas, origins, load_sem, out_sems):
    supers, groups, halves, edge, width = parts.shape
    depth, tall = canvas.shape[:2]
    chunk = tall // edge
    count = supers * groups
    lanes = 2 * edge
    steps = halves * count // chunk
    half = lax.broadcasted_iota(jnp.int32, (edge, lanes), 1) // edge
    load = pltpu.make_async_copy(parts_in, parts, load_sem)
    load.start()
    for n in range(depth):
        canvas[n] = jnp.zeros(canvas.shape[1:], canvas.dtype)

    @pl.loop(0, count)
    def _(n):
        origins[perm[n * panels] % count] = n

    residue = residue_of(perm, panels, count, lax.axis_index("col"))
    first = lax.axis_index("row") * halves
    late = [
        (residue < residue_of(perm, panels, count, first + e)).astype(jnp.int32)
        for e in range(halves)
    ]
    blank = jnp.zeros((edge, lanes), canvas.dtype)
    load.wait()

    def copy_of(step, slot):
        to = pl.ds(pl.multiple_of(step * tall, tall), tall)
        return pltpu.make_async_copy(canvas.at[slot], out.at[to], out_sems.at[slot])

    def lanes_of(block):
        return pl.ds(pl.multiple_of((block // 2) * lanes, lanes), lanes)

    def blocks_of(step, n):
        e = step * chunk // count
        origin = origins[lax.rem(step * chunk + n, count)]
        shift = late[0]
        for k in range(1, halves):
            shift = jnp.where(e == k, late[k], shift)
        base = origin - 2 + shift + count
        return e, origin, [
            perm[lax.rem(base + o, count) * panels] % count for o in range(width // edge)
        ]

    def fill(step, slot):
        for n in range(chunk):
            e, origin, blocks = blocks_of(step, n)
            at = slice(n * edge, (n + 1) * edge)
            made = []
            for w in range(width // lanes):
                tile = parts[
                    origin // groups, lax.rem(origin, groups), e, :, w * lanes : (w + 1) * lanes
                ].astype(jnp.float32)
                rolled = pltpu.roll(tile, edge, 1)
                for side in range(2):
                    odd = lax.rem(blocks[2 * w + side], 2)
                    value = jnp.where(odd == side, tile, rolled)
                    value = jnp.where(half == odd, value, 0.0).astype(canvas.dtype)
                    made.append((lanes_of(blocks[2 * w + side]), value))
            for to, value in made:
                canvas[slot, at, to] += value

    def clear(step, slot):
        for n in range(chunk):
            for block in blocks_of(step, n)[2]:
                canvas[slot, n * edge : (n + 1) * edge, lanes_of(block)] = blank

    @pl.loop(0, steps // depth)
    def _(r):
        for slot in range(depth):
            step = r * depth + slot

            @pl.when(r > 0)
            def _(step=step, slot=slot):
                copy_of(step - depth, slot).wait()
                clear(step - depth, slot)

            fill(step, slot)
            copy_of(step, slot).start()

    for slot in range(depth):
        copy_of(steps - depth + slot, slot).wait()


def place_blocks(parts, perm, panels):
    supers, groups, halves, edge, width = parts.shape
    count = supers * groups
    chunk, depth = 8, 4
    dma = pltpu.SemaphoreType.DMA
    return pl.pallas_call(
        functools.partial(place_kernel, panels),
        out_shape=jax.ShapeDtypeStruct((halves * count * edge, count * edge), parts.dtype),
        grid_spec=pltpu.PrefetchScalarGridSpec(
            num_scalar_prefetch=1,
            grid=(1,),
            in_specs=[ANY],
            out_specs=ANY,
            scratch_shapes=[
                pltpu.VMEM(parts.shape, parts.dtype),
                pltpu.VMEM((depth, chunk * edge, count * edge), parts.dtype),
                pltpu.SMEM((count,), jnp.int32),
                dma,
                dma((depth,)),
            ],
        ),
        compiler_params=pltpu.CompilerParams(dimension_semantics=("arbitrary",)),
        name="place_blocks",
    )(perm, parts)


def band_shards(x_vals, occupancy, perm):
    row_devices = lax.axis_size("row")
    panels = lax.axis_size("col")
    band = x_vals.shape[1]
    scale = 0.5 / (BLOCK_EDGE * band)
    parts = band_step(x_vals, occupancy, perm, row_devices, panels, scale)
    return place_blocks(parts, perm, panels)


def shards(x_vals, occupancy, perm):
    row_devices = lax.axis_size("row")
    panels = lax.axis_size("col")
    count, band, _ = x_vals.shape
    if row_devices == 4 and panels == count == 2 * row_devices and band == 4 * count:
        return band_shards(x_vals, occupancy, perm)
    return panel_shards(x_vals, occupancy, perm)


def solution(mesh):
    return jax.shard_map(
        shards,
        mesh=mesh,
        in_specs=(P(("row", "col"), None, None), P(("row", "col"), None), P()),
        out_specs=P("row", "col"),
        check_vma=False,
    )
```

```python
import functools

import jax
import jax.numpy as jnp
from jax import lax
from jax.experimental import pallas as pl
from jax.experimental.pallas import tpu as pltpu
from jax.sharding import PartitionSpec as P

BLOCK_EDGE = 64
MESH = pl.DeviceIdType.MESH
ANY = pl.BlockSpec(memory_space=pl.ANY)


def multiply_kernel(order_ref, left_ref, far0, far1, far2, far3, out_ref):
    width = out_ref.shape[-1]
    left = left_ref[...].reshape(-1, width)
    right = jnp.concatenate([r[...].reshape(-1, width) for r in (far0, far1, far2, far3)], axis=0)
    update = jnp.dot(left, right, preferred_element_type=jnp.float32).reshape(out_ref.shape)

    @pl.when(pl.program_id(1) == 0)
    def _():
        out_ref[...] = update

    @pl.when(pl.program_id(1) != 0)
    def _():
        out_ref[...] += update


def banded_product(left, far, order, residue_major, slots):
    panels, halves, count, edge, width = left.shape
    chunk = slots // 2
    chunks = count // chunk

    def far_spec(position):
        def chunk_of(g):
            return lax.rem(2 * g + chunks - 1 + lax.rem(position + 1 + 2 * g, 4), chunks)

        if residue_major:
            return pl.BlockSpec(
                (1, chunk, edge, width), lambda g, p, order: (order[p], chunk_of(g), 0, 0)
            )
        return pl.BlockSpec(
            (chunk, 1, edge, width), lambda g, p, order: (chunk_of(g), order[p], 0, 0)
        )

    return pl.pallas_call(
        multiply_kernel,
        out_shape=jax.ShapeDtypeStruct((halves, count, edge, width), jnp.float32),
        grid_spec=pltpu.PrefetchScalarGridSpec(
            num_scalar_prefetch=1,
            grid=(count // slots, panels),
            in_specs=[
                pl.BlockSpec(
                    (1, halves, slots, edge, width), lambda g, p, order: (p, 0, g, 0, 0)
                )
            ]
            + [far_spec(position) for position in range(4)],
            out_specs=pl.BlockSpec((halves, slots, edge, width), lambda g, p, order: (0, g, 0, 0)),
        ),
        compiler_params=pltpu.CompilerParams(dimension_semantics=("arbitrary", "arbitrary")),
    )(order, left, far, far, far, far)


def spread_kernel(source_ref, target_ref, rows_ref, out_ref):
    slots = rows_ref.shape[-1] // BLOCK_EDGE
    q, n = pl.program_id(0), pl.program_id(1)
    row = q * pl.num_programs(1) + source_ref[n]
    out_ref[...] = jnp.zeros_like(out_ref)
    for v in range(slots):
        block = rows_ref[0, 0, :, v * BLOCK_EDGE : (v + 1) * BLOCK_EDGE].astype(jnp.float32)
        target = target_ref[row * slots + v]
        odd = lax.rem(target, 2)
        pair = jnp.concatenate(
            [block * (1 - odd).astype(jnp.float32), block * odd.astype(jnp.float32)], axis=1
        ).astype(out_ref.dtype)
        at = pl.multiple_of((target // 2) * (2 * BLOCK_EDGE), 2 * BLOCK_EDGE)
        out_ref[:, pl.ds(at, 2 * BLOCK_EDGE)] += pair


def spread(rows, source, target, panel_cols):
    halves, count, edge, width = rows.shape
    return pl.pallas_call(
        spread_kernel,
        out_shape=jax.ShapeDtypeStruct((halves * count * edge, panel_cols * edge), rows.dtype),
        grid_spec=pltpu.PrefetchScalarGridSpec(
            num_scalar_prefetch=2,
            grid=(halves, count),
            in_specs=[
                pl.BlockSpec((1, 1, edge, width), lambda q, n, source, target: (q, source[n], 0, 0))
            ],
            out_specs=pl.BlockSpec(
                (edge, panel_cols * edge), lambda q, n, source, target: (q * count + n, 0)
            ),
        ),
        compiler_params=pltpu.CompilerParams(dimension_semantics=("arbitrary", "arbitrary")),
    )(source, target, rows)


def band_index(m, row_residue, col_residue, slots):
    first = m - slots // 2 + (col_residue < row_residue).astype(jnp.int32)
    v = jnp.arange(slots, dtype=jnp.int32)
    first = first[..., None]
    return first + (v - first) % slots


def widen(values, index, slots):
    high = (index % (2 * slots)) >= slots
    high = jnp.repeat(high, BLOCK_EDGE, axis=-1)[..., None, :]
    zero = jnp.zeros((), values.dtype)
    return jnp.concatenate(
        [jnp.where(high, zero, values), jnp.where(high, values, zero)], axis=-1
    )


def panel_shards(x_vals, occupancy, perm):
    row_devices = lax.axis_size("row")
    panels = lax.axis_size("col")
    own_row = lax.axis_index("row")
    own_col = lax.axis_index("col")
    local_rows, band_extent, block_area = x_vals.shape
    block_count = perm.shape[0]
    panel_cols = block_count // panels
    halves = panels // row_devices
    slots = band_extent // panels
    lanes = slots * BLOCK_EDGE

    panel_of_residue = perm[:panels] // panel_cols
    residue_ids = jnp.arange(panels, dtype=jnp.int32)
    order = jnp.sum(
        jnp.where(panel_of_residue[None, :] == residue_ids[:, None], residue_ids[None, :], 0), axis=1
    ).astype(jnp.int32)
    inside = perm[::panels] % panel_cols
    m_ids = jnp.arange(panel_cols, dtype=jnp.int32)
    source = jnp.sum(
        jnp.where(inside[None, :] == m_ids[:, None], m_ids[None, :], 0), axis=1
    ).astype(jnp.int32)
    own_residue = order[own_col]
    row_residues = lax.dynamic_slice_in_dim(order, own_row * halves, halves)

    first_row = (own_row * panels + own_col) * local_rows
    row_ids = first_row + jnp.arange(local_rows, dtype=jnp.int32)
    cols = (
        row_ids[:, None] - band_extent // 2 + jnp.arange(band_extent, dtype=jnp.int32)[None, :]
    ) % block_count
    placed = (
        (occupancy[:, :, None, None] == 1)
        & ((cols % panels)[:, :, None, None] == order[None, None, :, None])
        & (
            ((cols // panels) % slots)[:, :, None, None]
            == jnp.arange(slots, dtype=jnp.int32)[None, None, None, :]
        )
    ).astype(jnp.bfloat16)
    kept = jnp.sum(placed.astype(jnp.float32), axis=1).astype(jnp.bfloat16)
    every_kept = lax.all_gather(
        kept.reshape(local_rows, panels * slots), ("row", "col"), axis=0, tiled=True
    ).reshape(panel_cols, panels, panels, slots)
    values = jnp.einsum(
        "kspt,ksf->pktf", placed, x_vals, preferred_element_type=jnp.float32
    ).astype(jnp.bfloat16)
    values = (
        values.reshape(panels, local_rows, slots, BLOCK_EDGE, BLOCK_EDGE)
        .transpose(0, 1, 3, 2, 4)
        .reshape(panels, local_rows, BLOCK_EDGE, lanes)
    )
    first = lax.all_to_all(values, "col", split_axis=0, concat_axis=0, tiled=True)
    first = first.reshape(panels * local_rows, BLOCK_EDGE, lanes)
    far = lax.all_gather(first, "row", axis=0, tiled=True).reshape(
        panel_cols, panels, BLOCK_EDGE, lanes
    )
    tile = jnp.stack(
        [
            lax.dynamic_index_in_dim(far, row_residues[q], axis=1, keepdims=False)
            for q in range(halves)
        ]
    )
    own_kept = lax.dynamic_index_in_dim(every_kept, own_col, axis=2, keepdims=False)
    wanted = jnp.stack(
        [
            lax.dynamic_index_in_dim(own_kept, row_residues[q], axis=1, keepdims=False)
            for q in range(halves)
        ]
    )
    wanted = wanted > 0
    left = lax.all_gather(tile[None], "col", axis=0, tiled=True)

    far_index = band_index(m_ids[:, None], residue_ids[None, :], own_residue, slots)
    far_wide = widen(far, far_index, slots)
    left_index = band_index(
        m_ids[None, None, :], row_residues[None, :, None], order[:, None, None], slots
    )
    left_wide = widen(left, left_index, slots)
    tile_index = band_index(m_ids[None, :], row_residues[:, None], own_residue, slots)
    tile_high = (tile_index % (2 * slots)) >= slots

    def spread_mask(mask):
        return jnp.repeat(mask, BLOCK_EDGE, axis=-1)[:, :, None, :]

    def narrow(wide):
        chosen = jnp.where(spread_mask(tile_high), wide[..., lanes:], wide[..., :lanes])
        return jnp.where(spread_mask(wanted), chosen, 0.0)

    square = narrow(banded_product(left_wide, far_wide, order, False, slots)).astype(jnp.bfloat16)
    far_square = lax.all_gather(square, "row", axis=0, tiled=True)
    square_index = band_index(m_ids[None, :], order[:, None], own_residue, slots)
    square_wide = widen(far_square, square_index, slots)
    cube = narrow(banded_product(left_wide, square_wide, residue_ids, True, slots))
    stepped = (
        1.5 * tile.astype(jnp.float32) - 0.5 / (BLOCK_EDGE * band_extent) * cube
    ).astype(jnp.bfloat16)
    hit = (tile_index % panel_cols)[..., None] == m_ids
    target = jnp.sum(jnp.where(hit, inside, 0), axis=-1).astype(jnp.int32).reshape(-1)
    return spread(stepped, source, target, panel_cols)


class Place:
    def __init__(self, panels):
        self.depth = panels // 2
        self.quarter = panels // 4
        row, col = lax.axis_index("row"), lax.axis_index("col")
        self.half, self.core = row // 2, row % 2
        self.level, self.lane = col // 2, col % 2
        self.step = jnp.where(self.half == 0, self.level, self.depth - 1 - self.level)
        self.ring = self.half * self.depth + self.step

    def device(self, half, core, level, lane):
        return (2 * half + core, 2 * level + lane)

    def at_ring(self, ring):
        half = ring // self.depth
        step = ring % self.depth
        level = jnp.where(half == 0, step, self.depth - 1 - step)
        return self.device(half, self.core, level, self.lane)

    def neighbour(self, by):
        return self.at_ring((self.ring + by + 2 * self.depth) % (2 * self.depth))

    def group_target(self):
        step = self.core * self.quarter + self.level // 2
        level = jnp.where(self.half == 0, step, self.depth - 1 - step)
        return self.device(self.half, 1 - self.level % 2, level, self.lane)

    def group_source(self):
        level = 2 * (self.step % self.quarter) + 1 - self.core
        return self.device(self.half, self.step // self.quarter, level, self.lane)


def remote(source, target, send, recv, device):
    return pltpu.make_async_remote_copy(
        src_ref=source,
        dst_ref=target,
        send_sem=send,
        recv_sem=recv,
        device_id=device,
        device_id_type=MESH,
    )


def residue_of(perm, panels, panel_cols, spot):
    found = jnp.int32(0)
    for n in range(panels):
        found = found + jnp.where(perm[n] // panel_cols == spot, n, 0)
    return found


def core_kernel(
    panels, scale, present, perm, x_vals, flags, out,
    x_ref, rows, marks, pick, sort, late, mid, pairs,
    all_rows, all_marks, left, tiles, square, kept, total, sorted_rows, packed,
    move_sems, lane_sems, core_sems, relay_sems, halo_sems, square_sems, send, recv, local, load_sems,
):
    place = Place(panels)
    row, col = lax.axis_index("row"), lax.axis_index("col")
    count, edge, band_lanes = rows.shape
    octet = count * edge
    groups = all_rows.shape[0]
    wide, narrow = left.shape[-1], tiles.shape[-1]
    width = pick.shape[1]
    row_devices, pair = packed.shape[:2]
    halves = packed.shape[3]
    supers = out.shape[0]

    target, source = place.group_target(), place.group_source()
    lane_peer = place.device(place.half, place.core, place.level, 1 - place.lane)
    core_peer = place.device(place.half, 1 - place.core, place.level, place.lane)
    after, before = place.neighbour(1), place.neighbour(-1)
    target_slot = 2 * (place.level % 2) + place.lane
    own_slot = 2 * (1 - place.core) + place.lane
    peer_slot = 2 * (1 - place.core) + 1 - place.lane
    third_slot = 2 * place.core + place.lane
    last_slot = 2 * place.core + 1 - place.lane
    owner = place.level // 2
    senders = []
    for ring in range(supers):
        half, step = ring // place.depth, ring % place.depth
        level = step if half == 0 else place.depth - 1 - step
        senders.append((2 * half + owner, 2 * level + place.lane))
    receivers = [
        (dest, 2 * (2 * place.core + h) + place.lane)
        for dest in range(row_devices)
        for h in range(pair)
    ]

    def is_here(device):
        return jnp.logical_and(device[0] == row, device[1] == col)

    def load_of(t):
        return pltpu.make_async_copy(x_vals.at[t], x_ref.at[t], load_sems.at[t])

    @pl.loop(0, count)
    def _(t):
        load_of(t).start()

    barrier = pltpu.get_barrier_semaphore()
    for device in (source, lane_peer, core_peer, after, before):
        pl.semaphore_signal(barrier, inc=1, device_id=device, device_id_type=MESH)
    for device in senders:

        @pl.when(jnp.logical_not(is_here(device)))
        def _(device=device):
            pl.semaphore_signal(barrier, inc=1, device_id=device, device_id_type=MESH)

    def piece_of(ref, n):
        return ref.at[n // 2, pl.ds(n % 2 * (edge // 2), edge // 2)]

    def copy_of(n, sems, device, slot, first=False):
        landing = piece_of(all_rows.at[slot], n)
        origin = piece_of(rows, n) if first else landing
        return remote(origin, landing, sems.at[0, n], sems.at[1, n], device)

    def mark_of(sems, device, slot, first=False):
        origin = marks if first else all_marks.at[slot]
        return remote(
            origin, all_marks.at[slot], sems.at[0, 2 * count], sems.at[1, 2 * count], device
        )

    mark_copies = [
        mark_of(move_sems, target, target_slot, True),
        mark_of(lane_sems, lane_peer, own_slot),
        mark_of(core_sems, core_peer, own_slot),
        mark_of(relay_sems, core_peer, peer_slot),
    ]
    lanes = 2 * edge
    low = lax.broadcasted_iota(jnp.int32, (edge, lanes), 1) < edge
    panel_cols = perm.shape[0] // panels
    band, area = x_ref.shape[1:]
    tall = area // lanes
    pitch = mid.shape[0] // tall

    def relay_row(t):
        for p in range(tall):
            mid[p * pitch : p * pitch + band, :] = x_ref[
                t, :, p * lanes : (p + 1) * lanes
            ].astype(jnp.float32)
        for w in range(band // 2):
            one = mid[pl.ds(2 * w, tall, stride=pitch), :] * present[t, 2 * w].astype(jnp.float32)
            two = mid[pl.ds(2 * w + 1, tall, stride=pitch), :] * present[t, 2 * w + 1].astype(
                jnp.float32
            )
            lower = low[:tall]
            pairs[w, pl.ds(0, tall, stride=2), :] = jnp.where(
                lower, one, pltpu.roll(two, edge, 1)
            )
            pairs[w, pl.ds(1, tall, stride=2), :] = jnp.where(
                lower, pltpu.roll(one, edge, 1), two
            )
        for w in range(band // 2):
            rows[t, :, w * lanes : (w + 1) * lanes] = pairs[w].astype(rows.dtype)

    wide_flags = jnp.concatenate([flags[...].astype(jnp.float32)] * count, axis=1)
    at = (count, count * band)
    own = lax.broadcasted_iota(jnp.int32, at, 1) // band == lax.broadcasted_iota(jnp.int32, at, 0)
    to = (count * band, wide)
    entry, lane = (lax.broadcasted_iota(jnp.int32, to, n) for n in range(2))
    spread = (lane // edge - entry // band == entry % band).astype(jnp.float32)
    marks[...] = jnp.dot(
        jnp.where(own, wide_flags, 0.0).astype(marks.dtype),
        spread.astype(marks.dtype),
        preferred_element_type=jnp.float32,
    ).astype(marks.dtype)
    first = 4 * place.core + place.lane
    residues = [residue_of(perm, panels, panel_cols, first + 2 * h) for h in range(2)]
    entry, lane = (lax.broadcasted_iota(jnp.int32, pick.shape, n) for n in range(2))
    base = jnp.where(lane < edge, residues[0] * edge, (residues[1] - 1) * edge)
    pick[...] = (entry == base + lane).astype(jnp.float32).astype(pick.dtype)
    lane = lax.broadcasted_iota(jnp.int32, (1, lanes), 1)
    own = jnp.where(lane < edge, residues[0], residues[1])
    to, entry = (lax.broadcasted_iota(jnp.int32, (edge, octet), n) for n in range(2))
    for n in range(row_devices * halves):
        spot = residue_of(perm, panels, panel_cols, n)
        sort[n * edge : (n + 1) * edge, :] = (
            (entry == to + spot * edge).astype(jnp.float32).astype(sort.dtype)
        )
        late[n : n + 1, :] = (own < spot).astype(jnp.float32)

    load_of(0).wait()
    relay_row(0)
    expected = 5 + len(receivers)
    pl.semaphore_wait(barrier, jnp.where(owner == place.core, expected - 1, expected))

    mark_copies[0].start()

    @pl.loop(0, count + 1)
    def _(t):
        @pl.when(jnp.logical_and(t > 0, t < count))
        def _():
            load_of(t).wait()
            relay_row(t)

        @pl.when(t > 0)
        def _():
            for n in range(2):
                copy_of(2 * (t - 1) + n, move_sems, target, target_slot, True).start()

    @pl.loop(0, groups)
    def _(t):
        left[t] = jnp.zeros(left.shape[1:], left.dtype)

    def lay(slot, m):
        base = pl.multiple_of(2 * m * edge, 2 * edge)
        zeros = jnp.zeros((edge, edge), left.dtype)
        reach = pl.ds(base, band_lanes + 2 * edge)
        left[slot, pl.ds(base, edge), pl.ds(base, band_lanes)] = all_rows[slot, 2 * m]
        left[slot, pl.ds(pl.multiple_of(base + edge, edge), edge), reach] = jnp.concatenate(
            [zeros, all_rows[slot, 2 * m + 1], zeros], axis=1
        )
        chosen = pick[...]
        for o in range(wide // octet):
            tiles[slot + 2, pl.ds(base, 2 * edge), o * width : (o + 1) * width] = jnp.dot(
                left[slot, pl.ds(base, 2 * edge), o * octet : (o + 1) * octet],
                chosen,
                preferred_element_type=jnp.float32,
            ).astype(tiles.dtype)

    def halo(ref, sems):
        step = narrow // 5
        moves = (
            (groups + 1, 1, slice(step, narrow), after),
            (groups, 0, slice(2 * step, narrow), after),
            (2, groups + 2, slice(0, 4 * step), before),
            (3, groups + 3, slice(0, 3 * step), before),
        )
        return [
            remote(
                ref.at[origin, :, lanes], ref.at[to, :, lanes], sems.at[0, n], sems.at[1, n], device
            )
            for n, (origin, to, lanes, device) in enumerate(moves)
        ]

    first_halo = halo(tiles, halo_sems)
    sends = {1: 3, 0: 2, 2: 1, 3: 0}

    def send_tile(slot):
        for t in range(groups):

            @pl.when(slot == t)
            def _(t=t):
                first_halo[sends[t]].start()

    rounds = count // 2
    mark_copies[0].wait_recv()
    mark_copies[1].start()
    mark_copies[2].start()

    @pl.loop(0, rounds)
    def _(m):
        for i in range(4):
            n = 4 * m + i
            copy_of(n, move_sems, target, target_slot, True).wait_recv()
            copy_of(n, lane_sems, lane_peer, own_slot).start()
            copy_of(n, core_sems, core_peer, own_slot).start()
        lay(own_slot, m)

    send_tile(own_slot)
    mark_copies[1].wait_recv()
    mark_copies[3].start()

    @pl.loop(0, rounds)
    def _(m):
        for i in range(4):
            n = 4 * m + i
            copy_of(n, lane_sems, lane_peer, own_slot).wait_recv()
            copy_of(n, relay_sems, core_peer, peer_slot).start()
        for i in range(4):
            copy_of(4 * m + i, core_sems, core_peer, own_slot).wait_recv()
        lay(peer_slot, m)
        lay(third_slot, m)

    send_tile(peer_slot)
    send_tile(third_slot)
    @pl.loop(0, rounds)
    def _(m):
        for i in range(4):
            copy_of(4 * m + i, relay_sems, core_peer, peer_slot).wait_recv()
        lay(last_slot, m)

    send_tile(last_slot)

    mark_copies[2].wait_recv()
    mark_copies[3].wait_recv()
    for t in range(groups):
        for o in range(wide // octet):
            kept[t, :, o * width : (o + 1) * width] = jnp.dot(
                all_marks[t, :, o * octet : (o + 1) * octet],
                pick[...],
                preferred_element_type=jnp.float32,
            )

    def term(ref, t, by, fresh=False):
        step = narrow // 5
        reach = narrow - abs(by) * step
        first = 0 if by >= 0 else narrow - reach
        to = max(by, 0) * step
        update = jnp.dot(
            left[t, :, (2 + by) * octet : (3 + by) * octet],
            ref[t + 2 + by, :, first : first + reach],
            preferred_element_type=jnp.float32,
        )
        if fresh:
            total[t] = update
        else:
            total[t, :, to : to + reach] += update

    def own_terms(ref):
        @pl.loop(0, groups)
        def _(t):
            term(ref, t, 0, True)
            for by in (-2, -1, 1, 2):

                @pl.when(jnp.logical_and(t + by >= 0, t + by < groups))
                def _(by=by):
                    term(ref, t, by)

    def halo_terms(ref, t):
        for by in (-2, -1, 1, 2):
            if not 0 <= t + by < groups:
                term(ref, t, by)

    own_terms(tiles)
    second_halo = halo(square, square_sems)
    turns = (0, 3, 1, 2)
    reads = {0: (0, 1), 1: (0,), 2: (2,), 3: (2, 3)}
    waited = set()
    for t in turns:
        for n in reads[t]:
            if n not in waited:
                first_halo[n].wait_recv()
                waited.add(n)
        halo_terms(tiles, t)
        for r in range(count):
            at = slice(r * edge, (r + 1) * edge)
            square[t + 2, at, :] = (total[t, at, :] * kept[t, r : r + 1, :]).astype(square.dtype)
        second_halo[sends[t]].start()

    own_terms(square)
    turns = (2, 1, 3, 0)
    def delivery(t, n):
        dest, h = n // pair, n % pair
        return remote(
            packed.at[dest, h, t],
            out.at[place.ring, t],
            send.at[n, t],
            recv.at[place.ring, t],
            receivers[n],
        )

    def kept_here(t, n):
        return pltpu.make_async_copy(
            packed.at[n // pair, n % pair, t], out.at[place.ring, t], local.at[t]
        )

    def each_receiver(t, away, here):
        for n, device in enumerate(receivers):

            @pl.when(is_here(device))
            def _(n=n):
                here(kept_here(t, n))

            @pl.when(jnp.logical_not(is_here(device)))
            def _(n=n):
                away(delivery(t, n))

    waited = set()
    for t in turns:
        for n in reads[t]:
            if n not in waited:
                second_halo[n].wait_recv()
                waited.add(n)
        halo_terms(square, t)
        for r in range(count):
            at = slice(r * edge, (r + 1) * edge)
            total[t, at, :] = 1.5 * tiles[t + 2, at, :].astype(jnp.float32) - scale * (
                total[t, at, :] * kept[t, r : r + 1, :]
            )
        sorted_rows[...] = jnp.dot(
            sort[...], total[t].astype(packed.dtype), preferred_element_type=jnp.float32
        )
        for n in range(row_devices * halves):
            dest, e = n // halves, n % halves
            at = slice(n * edge, (n + 1) * edge)
            shift = late[n : n + 1, :] > 0.5
            parts = [sorted_rows[at, o * lanes : (o + 1) * lanes] for o in range(narrow // lanes)]
            parts = [jnp.where(shift, two, one) for one, two in zip(parts, parts[1:])]
            turned = [pltpu.roll(part, edge, 1) for part in parts]
            for w in range(len(parts) // 2):
                to = slice(w * lanes, (w + 1) * lanes)
                packed[dest, 0, t, e, :, to] = jnp.where(
                    low, parts[2 * w], turned[2 * w + 1]
                ).astype(packed.dtype)
                packed[dest, 1, t, e, :, to] = jnp.where(
                    low, turned[2 * w], parts[2 * w + 1]
                ).astype(packed.dtype)
        each_receiver(t, lambda copy: copy.start(), lambda copy: copy.start())

    for copy in mark_copies + first_halo + second_halo:
        copy.wait_send()

    @pl.loop(0, 2 * count)
    def _(n):
        copy_of(n, move_sems, target, target_slot, True).wait_send()
        copy_of(n, lane_sems, lane_peer, own_slot).wait_send()
        copy_of(n, core_sems, core_peer, own_slot).wait_send()
        copy_of(n, relay_sems, core_peer, peer_slot).wait_send()

    for t in turns:
        for n, device in enumerate(senders):

            @pl.when(jnp.logical_not(is_here(device)))
            def _(t=t, n=n, device=device):
                remote(
                    packed.at[0, 0, t], out.at[n, t], send.at[0, t], recv.at[n, t], device
                ).wait_recv()

        each_receiver(t, lambda copy: copy.wait_send(), lambda copy: copy.wait())


def band_step(x_vals, occupancy, perm, row_devices, panels, scale):
    count, band, area = x_vals.shape
    edge = BLOCK_EDGE
    lanes = 2 * edge
    octet, wide = count * edge, (band + count) * edge
    narrow = wide // octet * lanes
    halves = panels // row_devices
    supers = perm.shape[0] // (4 * count)
    kind = x_vals.dtype
    rows = (count, edge, band * edge)
    out = (supers, 4, halves, edge, 4 * edge)
    dma = pltpu.SemaphoreType.DMA
    vmem = pl.BlockSpec(memory_space=pltpu.VMEM)
    smem = pl.BlockSpec(memory_space=pltpu.SMEM)
    return pl.pallas_call(
        functools.partial(core_kernel, panels, scale),
        out_shape=jax.ShapeDtypeStruct(out, kind),
        in_specs=[smem, smem, ANY, vmem],
        out_specs=ANY,
        scratch_shapes=[
            pltpu.VMEM(x_vals.shape, kind),
            pltpu.VMEM(rows, kind),
            pltpu.VMEM((count, wide), kind),
            pltpu.VMEM((octet, lanes), kind),
            pltpu.VMEM((octet, octet), kind),
            pltpu.VMEM((count, lanes), jnp.float32),
            pltpu.VMEM((area // lanes * (band + 8), lanes), jnp.float32),
            pltpu.VMEM((band // 2, edge, lanes), jnp.float32),
            pltpu.VMEM((4,) + rows, kind),
            pltpu.VMEM((4, count, wide), kind),
            pltpu.VMEM((4, octet, wide), kind),
            pltpu.VMEM((8, octet, narrow), kind),
            pltpu.VMEM((8, octet, narrow), kind),
            pltpu.VMEM((4, count, narrow), jnp.float32),
            pltpu.VMEM((4, octet, narrow), jnp.float32),
            pltpu.VMEM((octet, narrow), jnp.float32),
            pltpu.VMEM((row_devices, 2) + out[1:], kind),
            dma((2, 2 * count + 1)),
            dma((2, 2 * count + 1)),
            dma((2, 2 * count + 1)),
            dma((2, 2 * count + 1)),
            dma((2, 4)),
            dma((2, 4)),
            dma((2 * row_devices, 4)),
            dma((supers, 4)),
            dma((4,)),
            dma((count,)),
        ],
        compiler_params=pltpu.CompilerParams(
            collective_id=0, has_side_effects=True, vmem_limit_bytes=60 * 2**20
        ),
        name="band_step",
    )(occupancy, perm, x_vals, occupancy)


def place_kernel(panels, perm, parts_in, out, parts, canvas, origins, load_sem, out_sems):
    supers, groups, halves, edge, width = parts.shape
    depth, tall = canvas.shape[:2]
    chunk = tall // edge
    count = supers * groups
    lanes = 2 * edge
    steps = halves * count // chunk
    half = lax.broadcasted_iota(jnp.int32, (edge, lanes), 1) // edge
    load = pltpu.make_async_copy(parts_in, parts, load_sem)
    load.start()
    for n in range(depth):
        canvas[n] = jnp.zeros(canvas.shape[1:], canvas.dtype)

    @pl.loop(0, count)
    def _(n):
        origins[perm[n * panels] % count] = n

    residue = residue_of(perm, panels, count, lax.axis_index("col"))
    first = lax.axis_index("row") * halves
    late = [
        (residue < residue_of(perm, panels, count, first + e)).astype(jnp.int32)
        for e in range(halves)
    ]
    blank = jnp.zeros((edge, lanes), canvas.dtype)
    load.wait()

    def copy_of(step, slot):
        to = pl.ds(pl.multiple_of(step * tall, tall), tall)
        return pltpu.make_async_copy(canvas.at[slot], out.at[to], out_sems.at[slot])

    def lanes_of(block):
        return pl.ds(pl.multiple_of((block // 2) * lanes, lanes), lanes)

    def blocks_of(step, n):
        e = step * chunk // count
        origin = origins[lax.rem(step * chunk + n, count)]
        shift = late[0]
        for k in range(1, halves):
            shift = jnp.where(e == k, late[k], shift)
        base = origin - 2 + shift + count
        return e, origin, [
            perm[lax.rem(base + o, count) * panels] % count for o in range(width // edge)
        ]

    def fill(step, slot):
        for n in range(chunk):
            e, origin, blocks = blocks_of(step, n)
            at = slice(n * edge, (n + 1) * edge)
            made = []
            for w in range(width // lanes):
                tile = parts[
                    origin // groups, lax.rem(origin, groups), e, :, w * lanes : (w + 1) * lanes
                ].astype(jnp.float32)
                rolled = pltpu.roll(tile, edge, 1)
                for side in range(2):
                    odd = lax.rem(blocks[2 * w + side], 2)
                    value = jnp.where(odd == side, tile, rolled)
                    value = jnp.where(half == odd, value, 0.0).astype(canvas.dtype)
                    made.append((lanes_of(blocks[2 * w + side]), value))
            for to, value in made:
                canvas[slot, at, to] += value

    def clear(step, slot):
        for n in range(chunk):
            for block in blocks_of(step, n)[2]:
                canvas[slot, n * edge : (n + 1) * edge, lanes_of(block)] = blank

    @pl.loop(0, steps // depth)
    def _(r):
        for slot in range(depth):
            step = r * depth + slot

            @pl.when(r > 0)
            def _(step=step, slot=slot):
                copy_of(step - depth, slot).wait()
                clear(step - depth, slot)

            fill(step, slot)
            copy_of(step, slot).start()

    for slot in range(depth):
        copy_of(steps - depth + slot, slot).wait()


def place_blocks(parts, perm, panels):
    supers, groups, halves, edge, width = parts.shape
    count = supers * groups
    chunk, depth = 4, 16
    dma = pltpu.SemaphoreType.DMA
    return pl.pallas_call(
        functools.partial(place_kernel, panels),
        out_shape=jax.ShapeDtypeStruct((halves * count * edge, count * edge), parts.dtype),
        grid_spec=pltpu.PrefetchScalarGridSpec(
            num_scalar_prefetch=1,
            grid=(1,),
            in_specs=[ANY],
            out_specs=ANY,
            scratch_shapes=[
                pltpu.VMEM(parts.shape, parts.dtype),
                pltpu.VMEM((depth, chunk * edge, count * edge), parts.dtype),
                pltpu.SMEM((count,), jnp.int32),
                dma,
                dma((depth,)),
            ],
        ),
        compiler_params=pltpu.CompilerParams(dimension_semantics=("arbitrary",)),
        name="place_blocks",
    )(perm, parts)


def band_shards(x_vals, occupancy, perm):
    row_devices = lax.axis_size("row")
    panels = lax.axis_size("col")
    band = x_vals.shape[1]
    scale = 0.5 / (BLOCK_EDGE * band)
    parts = band_step(x_vals, occupancy, perm, row_devices, panels, scale)
    return place_blocks(parts, perm, panels)


def shards(x_vals, occupancy, perm):
    row_devices = lax.axis_size("row")
    panels = lax.axis_size("col")
    count, band, _ = x_vals.shape
    if row_devices == 4 and panels == count == 2 * row_devices and band == 4 * count:
        return band_shards(x_vals, occupancy, perm)
    return panel_shards(x_vals, occupancy, perm)


def solution(mesh):
    return jax.shard_map(
        shards,
        mesh=mesh,
        in_specs=(P(("row", "col"), None, None), P(("row", "col"), None), P()),
        out_specs=P("row", "col"),
        check_vma=False,
    )
```
